32 devices in a mesh: row: 4 (over z), col: 8 (over y, x, core).
Axes of the slice: x: 2, y: 2, z: 4, core: 2. Of those that a mesh axis runs over, the one named last changes fastest.
Arguments:
- load_amp: float32 [2048, 4096], P('row', 'col'), may hold values from 0.05 to 1
- load_mask: int32 [2048, 4096], P('row', 'col'), may hold values 0 or 1
- leak: float32 [2048, 4096], P('row', 'col'), may hold values from 0.001 to 0.05
- coarse_leak: float32 [512, 1024], P('row', 'col'), may hold values from 0.01 to 0.5
- coarse_init: float32 [512, 1024], P('row', 'col'), may hold values from 0 to 1
- via_fine: int32 [4, 8192], P('row', 'col'), may hold values from 0 to 262143
- via_coarse: int32 [4, 8192], P('row', 'col'), may hold values from 0 to 131071, as said below
- via_count: int32 [4, 64], P('row', 'col'), may hold values from 0 to 128, as said below
Outputs:
- fine_drop: float32 [2048, 4096], P('row', 'col')
- coarse_drop: float32 [512, 1024], P('row', 'col')
The draws below stay inside these ranges and needn't reach their ends.
Inputs may be any that keep to these rules, and one draw needn't show every extreme that they name: `via_coarse`: slot s of a tile names a coarse node whose stored column lies in s // 128 * 128 to s // 128 * 128 + 127. `via_count`: slots of an owner past its count are padding and carry arbitrary indices. In each tile row some owner gets 128 live slots from every tile of that row.
All inputs are finite; a program needn't handle non-finite values. No bound on the sum of `load_mask` on one device may be relied on, other than what follows from the above.
Results may differ from the reference program's by a relative error of at most 0.00022.
Values sent between devices are 32-bit elements; how exact they have to be, the bound alone decides.
A program may use at most 64 MiB of HBM per device.

```python
import math
import jax
import jax.numpy as jnp

FR = 512
FC = 512
CR = 128
CC = 128
GROUP = 16
VOWN = 128
ITERS = 4
OUTER = 1
CSWEEP = 2
NFR = 2048
NFC = 4096
NCR = 512
NCC = 1024
VMAX = 1024
N_ROW = 4
N_COL = 8


def draw_via_coarse(key, part):
    columns = NCC // CC
    tiles_down = NCR // CR
    slot_all = jnp.arange(columns * VMAX, dtype=jnp.int32)
    owner = slot_all % VMAX // VOWN
    key_row, key_col = jax.random.split(jax.random.fold_in(key, 11))
    shape = (tiles_down, columns * VMAX)
    row_pick = jax.random.randint(key_row, shape, 0, CR, dtype=jnp.int32)
    col_pick = jax.random.randint(key_col, shape, 0, CC, dtype=jnp.int32)
    return (row_pick * NCC + owner[None, :] * CC + col_pick).astype(jnp.int32)


def draw_via_count(key, part):
    columns = NCC // CC
    tiles_down = NCR // CR
    key_base, key_full = jax.random.split(jax.random.fold_in(key, 23))
    base = jax.random.randint(key_base, (tiles_down, columns * columns), 0, VOWN + 1, dtype=jnp.int32)
    chosen = jax.random.randint(key_full, (tiles_down, 1), 0, columns, dtype=jnp.int32)
    owner = jnp.arange(columns * columns, dtype=jnp.int32) % columns
    return jnp.where(owner[None, :] == chosen, VOWN, base).astype(jnp.int32)


def touch_ends(array, stream_key, low, high):
    shape = array.shape
    place = [jax.random.randint(jax.random.fold_in(stream_key, axis), (), 0, shape[axis]) for axis in range(len(shape))]
    array = array.at[tuple(place)].set(low)
    longest = shape.index(max(shape))
    place[longest] = (place[longest] + 1) % shape[longest]
    return array.at[tuple(place)].set(high)


def levels(own_key, dims, cuts, low, top_value):
    level, own = 1.0, jax.random.fold_in(own_key, 6)
    for dim, blocks in cuts:
        draws = jnp.exp(jax.random.uniform(jax.random.fold_in(own, dim), (blocks,), jnp.float32, low / len(cuts), top_value / len(cuts)))
        level = level * jnp.repeat(draws, dims[dim] // blocks).reshape([-1 if axis == dim else 1 for axis in range(len(dims))])
    return level


def setup_inputs(seed: int = 0) -> dict:
    key_of = jax.random.split(jax.random.key(seed), 9)
    load_amp = jnp.clip(jnp.exp(math.log(1.0) - 2.9957323 * jax.random.uniform(key_of[0], (NFR, NFC), jnp.float32) ** levels(key_of[0], (NFR, NFC), ((0, 4), (1, 8)), -0.2, 0.2)), 0.05, 1.0)
    load_mask = touch_ends((jax.random.randint(key_of[1], (NFR, NFC), 0, 2) < 1).astype(jnp.int32), jax.random.fold_in(key_of[1], 1), 0, 1)
    leak = jnp.clip(jnp.exp(math.log(0.05) - 3.912023 * jax.random.uniform(key_of[2], (NFR, NFC), jnp.float32) ** levels(key_of[2], (NFR, NFC), ((0, 4), (1, 8)), -0.2, 0.2)), 0.001, 0.05)
    coarse_leak = jnp.clip(jnp.exp(math.log(0.5) - 3.912023 * jax.random.uniform(key_of[3], (NCR, NCC), jnp.float32) ** levels(key_of[3], (NCR, NCC), ((0, 4), (1, 8)), -0.2, 0.2)), 0.01, 0.5)
    coarse_init = jnp.clip(1.0 * jax.random.uniform(key_of[4], (NCR, NCC), jnp.float32) ** levels(key_of[4], (NCR, NCC), ((0, 4), (1, 8)), -0.2, 0.2), 0.0, 1.0)
    via_fine = touch_ends(jax.random.randint(key_of[5], (N_ROW, VMAX * N_COL), 0, FR * FC), jax.random.fold_in(key_of[5], 1), 0, (FR * FC) - 1).astype(jnp.int32)
    via_coarse = draw_via_coarse(jax.random.fold_in(key_of[8], 71), 0)
    via_count = draw_via_count(jax.random.fold_in(key_of[8], 71), 0)
    return {"load_amp": load_amp, "load_mask": load_mask, "leak": leak, "coarse_leak": coarse_leak, "coarse_init": coarse_init, "via_fine": via_fine, "via_coarse": via_coarse, "via_count": via_count}


via_conductance = 2.0
coarse_conductance = 4.0
relaxation = 0.8


def fine_apply(field, diagonal):
    padded = jnp.pad(field, 1)
    beside = padded[2:, 1:-1] + padded[:-2, 1:-1] + padded[1:-1, 2:] + padded[1:-1, :-2]
    return diagonal * field - beside


def to_physical(stored):
    return stored.reshape(NCR, N_COL, CC // GROUP, GROUP).transpose(0, 2, 1, 3).reshape(NCR, NCC)


def to_stored(physical):
    return physical.reshape(NCR, CC // GROUP, N_COL, GROUP).transpose(0, 2, 1, 3).reshape(NCR, NCC)


def coarse_apply(stored, diagonal):
    padded = jnp.pad(to_physical(stored), 1)
    beside = padded[2:, 1:-1] + padded[:-2, 1:-1] + padded[1:-1, 2:] + padded[1:-1, :-2]
    return diagonal * stored - coarse_conductance * to_stored(beside)


def reference(load_amp, load_mask, leak, coarse_leak, coarse_init, via_fine, via_coarse, via_count):
    tile_row = jnp.arange(N_ROW, dtype=jnp.int32)[:, None]
    slot_all = jnp.arange(N_COL * VMAX, dtype=jnp.int32)[None, :]
    tile_col = slot_all // VMAX
    within = slot_all % VMAX
    owner = within // VOWN
    position = within % VOWN
    count_index = jnp.broadcast_to(tile_col * N_COL + owner, via_fine.shape).astype(jnp.int32)
    counts = jnp.take_along_axis(via_count, count_index, axis=1)
    weight = jnp.where(position < counts, via_conductance, 0.0).astype(jnp.float32).reshape(-1)
    fine_index = ((tile_row * FR + via_fine // FC) * NFC + tile_col * FC + via_fine % FC).reshape(-1)
    coarse_index = ((tile_row * CR + via_coarse // NCC) * NCC + via_coarse % NCC).reshape(-1)
    fine_diag = 4.0 + leak + jnp.zeros(NFR * NFC, jnp.float32).at[fine_index].add(weight).reshape(NFR, NFC)
    coarse_diag = 4.0 * coarse_conductance + coarse_leak + jnp.zeros(NCR * NCC, jnp.float32).at[coarse_index].add(weight).reshape(NCR, NCC)
    load = load_amp * load_mask.astype(jnp.float32)
    volt = coarse_init
    solution = jnp.zeros((NFR, NFC), jnp.float32)
    for outer_turn in range(OUTER):
        at_via = volt.reshape(-1)[coarse_index]
        rhs = load + jnp.zeros(NFR * NFC, jnp.float32).at[fine_index].add(weight * at_via).reshape(NFR, NFC)
        residual = rhs - fine_apply(solution, fine_diag)
        precond = residual / fine_diag
        direction = precond
        product = jnp.sum(residual * precond)
        for iteration in range(ITERS):
            image = fine_apply(direction, fine_diag)
            alpha = product / jnp.sum(direction * image)
            solution = solution + alpha * direction
            residual = residual - alpha * image
            if iteration + 1 < ITERS:
                precond = residual / fine_diag
                renewed = jnp.sum(residual * precond)
                direction = precond + (renewed / product) * direction
                product = renewed
        at_fine = weight * solution.reshape(-1)[fine_index]
        sources = jnp.zeros(NCR * NCC, jnp.float32).at[coarse_index].add(at_fine).reshape(NCR, NCC)
        for sweep_turn in range(CSWEEP):
            volt = volt + relaxation * (sources - coarse_apply(volt, coarse_diag)) / coarse_diag
    return solution, volt
```

```python
import functools
import jax
import jax.numpy as jnp
from jax import lax
from jax.experimental import pallas as pl
from jax.experimental.pallas import tpu as pltpu
from jax.sharding import PartitionSpec as P

GROUP = 16
ITERS = 4
LANES = 128
PAD = 16
EDGE = 8
HALF = LANES // 2
QUARTER = LANES // 4

via_conductance = 2.0
coarse_conductance = 4.0
relaxation = 0.8

F32 = jnp.float32
BF16 = jnp.bfloat16
MESH = pl.DeviceIdType.MESH


def divide(value, by):
    if by & (by - 1) == 0:
        return lax.shift_right_logical(value, by.bit_length() - 1)
    return value // by


def remainder(value, by):
    if by & (by - 1) == 0:
        return value & (by - 1)
    return value % by


def halves(value):
    high = value.astype(BF16).astype(F32)
    return high.astype(BF16), (value - high).astype(BF16)


def dot(a, b):
    return jnp.dot(a, b, preferred_element_type=F32)


def dot_t(a, b):
    return lax.dot_general(a, b, (((1,), (1,)), ((), ())), preferred_element_type=F32)


def fold(value):
    total = value[0:8]
    for n in range(1, value.shape[0] // 8):
        total = total + value[n * 8 : (n + 1) * 8]
    return total


def iota(shape, dim):
    return lax.broadcasted_iota(jnp.int32, shape, dim)


def kernel(
    R, C,
    amp_in, mask_in, leak_in, cleak_in, cinit_in, vf_in, vc_in, cnt_in,
    x_out, c_out,
    amp, mask, leak, cleak, cinit, vf, vc, cnt, load_sem,
    msg_out, msg_row, msg_ud, val_out, val_in, seen_out, seen_row, seen_ud,
    spot_v, spot, picked, lane_hot,
    row_hot, Bt, dv, D, dvq, Dq, V, Q, R0, rhs, rhsq,
    E, ET, H, rtop, rbot, rcorner,
    red_out, red_in,
    hot_own, hot_left, hot_right, hot_up, hot_down,
    coarse, turn, seam_out, crow_top, crow_bot, cleft, cright,
    send_sem, recv_sem,
):
    row, col = lax.axis_index("row"), lax.axis_index("col")
    TR, TC = leak_in.shape
    NB = TC // LANES
    EXT = TR + 2 * PAD
    BR, BC = cleak.shape
    S = vf.shape[1]
    per = S // C
    groups = BC // GROUP

    def cut(b):
        return pl.ds(b * LANES, LANES)

    loads = []

    def load(source, target):
        copy = pltpu.make_async_copy(source, target, load_sem.at[len(loads)])
        copy.start()
        loads.append(copy)
        return copy

    small = [load(cnt_in, cnt), load(vc_in, vc), load(vf_in, vf)]
    cinit_load = load(cinit_in, cinit)
    leak_loads = [load(leak_in.at[:, cut(b)], leak.at[b]) for b in range(NB)]
    cleak_load = load(cleak_in, cleak)
    amp_loads = [load(amp_in.at[:, cut(b)], amp.at[b]) for b in range(NB)]
    amp_loads += [load(mask_in.at[:, cut(b)], mask.at[b]) for b in range(NB)]

    up, down = lax.rem(row + R - 1, R), lax.rem(row + 1, R)
    left, right = lax.rem(col + C - 1, C), lax.rem(col + 1, C)
    top_ok, bot_ok = row > 0, row < R - 1
    left_ok, right_ok = col > 0, col < C - 1
    always = None

    barrier = pltpu.get_barrier_semaphore()

    def greet(r, c):
        pl.semaphore_signal(barrier, inc=1, device_id=(r, c), device_id_type=MESH)

    for d in range(1, C):
        greet(row, lax.rem(col + d, C))
    near_rows = R <= 4
    if near_rows:

        @pl.when(top_ok)
        def _():
            for d in range(C):
                greet(up, lax.rem(col + d, C))

        @pl.when(bot_ok)
        def _():
            for d in range(C):
                greet(down, lax.rem(col + d, C))
    else:
        for e in range(1, R):
            for d in range(C):
                greet(lax.rem(row + e, R), lax.rem(col + d, C))

    def welcome():
        if near_rows:
            rows = jnp.where(top_ok, 1, 0) + jnp.where(bot_ok, 1, 0)
            pl.semaphore_wait(barrier, C - 1 + C * rows)
        else:
            pl.semaphore_wait(barrier, R * C - 1)

    count = [0]
    pending = []

    def under(ok, body):
        if ok is always:
            body()
        else:
            pl.when(ok)(body)

    class Batch:
        def __init__(self, ok, heard, specs):
            self.ok, self.heard = ok, heard
            self.copies = []
            for src, dst, device in specs:
                n = count[0]
                count[0] += 1
                self.copies.append(pltpu.make_async_remote_copy(
                    src_ref=src, dst_ref=dst, send_sem=send_sem.at[n], recv_sem=recv_sem.at[n],
                    device_id=device, device_id_type=MESH,
                ))
            pending.append(self)

            def start():
                for copy in self.copies:
                    copy.start()

            under(ok, start)

        def land(self, otherwise=None):
            def wait():
                for copy in self.copies:
                    copy.wait_recv()

            under(self.heard, wait)
            if self.heard is not always and otherwise is not None:
                pl.when(jnp.logical_not(self.heard))(otherwise)

        def leave(self):
            def wait():
                for copy in self.copies:
                    copy.wait_send()

            under(self.ok, wait)

    for n in range(2):
        H[n] = jnp.zeros((LANES, TR), F32)
    for copy in small:
        copy.wait()
    lane = iota((1, per), 1)
    weight = jnp.concatenate(
        [jnp.where(lane < cnt[0, o], via_conductance, 0.0).astype(F32) for o in range(C)], axis=1
    )
    node = vc[...].astype(F32)
    for o in [-1] + list(range(C)) + [C]:
        part = slice((o % C) * per, (o % C + 1) * per)
        msg_out[o + 1, 0:1, :] = node[:, part]
        msg_out[o + 1, 1:2, :] = weight[:, part]
    msg_row[col] = msg_out[pl.ds(col, 3)]
    fine = vf[...]
    fine_row = divide(fine, TC)
    fine_col = remainder(fine, TC)
    spot_v[...] = divide(fine_col, LANES) * EXT + PAD + fine_row
    spot_copy = pltpu.make_async_copy(spot_v, spot, load_sem.at[len(loads)])
    spot_copy.start()
    step = 64

    def build_rows(i, carry):
        at = pl.ds(pl.multiple_of(i * step, step), step)
        place = iota((step, S), 0) + i * step
        row_hot[at, :] = jnp.where(place == fine_row, 1.0, 0.0).astype(BF16)
        return carry

    lax.fori_loop(0, TR // step, build_rows, 0)

    welcome()

    messages = Batch(always, always, [
        (msg_out.at[pl.ds(lax.rem(col + d, C), 3)], msg_row.at[col], (row, lax.rem(col + d, C)))
        for d in range(1, C)
    ])

    def seams(volt, n):
        turn[n] = volt.T
        seam_out[n, 0] = turn[n, pl.ds(0, groups, stride=GROUP), :]
        seam_out[n, 1] = turn[n, pl.ds(GROUP - 1, groups, stride=GROUP), :]

    def coarse_send(ref, n):
        return [
            Batch(top_ok, bot_ok, [(ref.at[pl.ds(0, 8)], crow_bot.at[n], (up, col))]),
            Batch(bot_ok, top_ok, [(ref.at[pl.ds(BR - 8, 8)], crow_top.at[n], (down, col))]),
            Batch(always, always, [
                (seam_out.at[n, 0], cright.at[n], (row, left)),
                (seam_out.at[n, 1], cleft.at[n], (row, right)),
            ]),
        ]

    def coarse_land(batches, n):
        def no_below():
            crow_bot[n] = jnp.zeros((8, BC), F32)

        def no_above():
            crow_top[n] = jnp.zeros((8, BC), F32)

        batches[0].land(no_below)
        batches[1].land(no_above)
        batches[2].land()

    cinit_load.wait()
    seams(cinit[...], 0)
    coarse0 = coarse_send(cinit, 0)
    messages_up = Batch(top_ok, bot_ok, [
        (msg_out.at[lax.rem(col + d, C) + 1], msg_ud.at[1, col], (up, lax.rem(col + d, C)))
        for d in range(C)
    ])
    messages_down = Batch(bot_ok, top_ok, [
        (msg_out.at[lax.rem(col + d, C) + 1], msg_ud.at[0, col], (down, lax.rem(col + d, C)))
        for d in range(C)
    ])

    lanes = iota((per, LANES), 1).astype(F32)
    for o in range(C):
        part = slice(o * per, (o + 1) * per)
        turned = jnp.broadcast_to(fine_col[:, part].astype(F32), (LANES, per)).T
        near = turned
        total = jnp.zeros((per, LANES), F32)
        for b in range(NB):
            hot = jnp.where(turned == lanes + b * LANES, 1.0, 0.0)
            Bt[part, b * LANES : (b + 1) * LANES] = hot.astype(BF16)
            total = total + hot
        lane_hot[part, :] = total

    zero_pad = jnp.zeros((8, LANES), F32)
    for n in range(ITERS):
        for b in range(NB):
            V[n, b * EXT : b * EXT + 8, :] = zero_pad
            V[n, (b + 1) * EXT - 8 : (b + 1) * EXT, :] = zero_pad
        for b in range(NB if n == 0 else 0):
            V[n, b * EXT + 8 : b * EXT + 16, :] = zero_pad
            V[n, (b + 1) * EXT - 16 : (b + 1) * EXT - 8, :] = zero_pad
        Q[n, 0:8, :] = zero_pad
        Q[n, EXT - 8 : EXT, :] = zero_pad
    for n in range(1, ITERS):
        for b in range(NB):
            V[n, b * EXT + 8 : b * EXT + 16, :] = zero_pad
            V[n, (b + 1) * EXT - 16 : (b + 1) * EXT - 8, :] = zero_pad

    for copy in leak_loads:
        copy.wait()
    wide_step = 256 if TR % 256 == 0 else step
    weight_low = weight.astype(BF16)

    def diagonal(i, carry):
        at = pl.ds(pl.multiple_of(i * wide_step, wide_step), wide_step)
        sums = dot(row_hot[at, :] * weight_low, Bt[...])
        for b in range(NB):
            inner = pl.ds(pl.multiple_of(b * EXT + PAD + i * wide_step, 8), wide_step)
            own = pl.ds(pl.multiple_of(b * TR + i * wide_step, 8), wide_step)
            value = 4.0 + leak[b, at, :] + sums[:, b * LANES : (b + 1) * LANES]
            D[own, :] = value
            dv[inner, :] = 1.0 / value
        return carry

    lax.fori_loop(0, TR // wide_step, diagonal, 0)

    lane_row = iota((8, LANES), 1)

    def wide(rows):
        return iota((rows, LANES), 1)

    def keep(ok, value):
        return value * jnp.where(ok, 1.0, 0.0).astype(F32)

    last = (NB - 1) * EXT

    def halo_send(F, n):
        edge = jnp.where(wide(TR) < HALF, F[PAD : PAD + TR, :], F[last + PAD : last + PAD + TR, :])
        E[n] = edge
        ET[n] = edge.T
        ends = [(PAD, up), (PAD + TR - EDGE, down)]
        sides = Batch(always, always, [
            (ET.at[n, pl.ds(0, EDGE)], H.at[n, pl.ds(HALF, EDGE)], (row, left)),
            (ET.at[n, pl.ds(LANES - EDGE, EDGE)], H.at[n, pl.ds(LANES - EDGE, EDGE)], (row, right)),
        ])
        above = Batch(top_ok, bot_ok, [
            (E.at[n, pl.ds(0, EDGE)], rcorner.at[n, 3], (up, left)),
            (E.at[n, pl.ds(0, EDGE)], rcorner.at[n, 2], (up, right)),
        ] + [
            (F.at[pl.ds(b * EXT + PAD, EDGE)], rbot.at[n, b], (up, col)) for b in range(NB)
        ])
        below = Batch(bot_ok, top_ok, [
            (E.at[n, pl.ds(TR - EDGE, EDGE)], rcorner.at[n, 1], (down, left)),
            (E.at[n, pl.ds(TR - EDGE, EDGE)], rcorner.at[n, 0], (down, right)),
        ] + [
            (F.at[pl.ds(b * EXT + PAD + TR - EDGE, EDGE)], rtop.at[n, b], (down, col)) for b in range(NB)
        ])
        return sides, above, below

    def edges_of(first, final, beyond):
        rows = first.shape[0]
        place = wide(rows)
        own = jnp.where(place < QUARTER, first, pltpu.roll(final, HALF, 1))
        if beyond is None:
            return own
        return jnp.where(place < HALF, own, beyond)

    def outer(right_side, left_side):
        place = wide(right_side.shape[0])
        return jnp.where(place < HALF + QUARTER, keep(right_ok, right_side), keep(left_ok, left_side))

    def halo_land(F, X, n, batches):
        sides, above, below = batches
        sides.land()
        side = H[n].T
        X[PAD : PAD + TR, :] = edges_of(
            F[PAD : PAD + TR, :], F[last + PAD : last + PAD + TR, :], outer(side, side)
        )

        def no_below():
            for b in range(NB):
                F[b * EXT + PAD + TR : b * EXT + PAD + TR + EDGE, :] = zero_pad
            X[PAD + TR : PAD + TR + EDGE, :] = zero_pad

        def no_above():
            for b in range(NB):
                F[b * EXT + PAD - EDGE : b * EXT + PAD, :] = zero_pad
            X[PAD - EDGE : PAD, :] = zero_pad

        above.land(no_below)
        below.land(no_above)

        @pl.when(bot_ok)
        def _():
            for b in range(NB):
                F[b * EXT + PAD + TR : b * EXT + PAD + TR + EDGE, :] = rbot[n, b]
            beyond = outer(pltpu.roll(rcorner[n, 3], HALF, 1), rcorner[n, 2])
            X[PAD + TR : PAD + TR + EDGE, :] = edges_of(rbot[n, 0], rbot[n, NB - 1], beyond)

        @pl.when(top_ok)
        def _():
            for b in range(NB):
                F[b * EXT + PAD - EDGE : b * EXT + PAD, :] = rtop[n, b]
            beyond = outer(pltpu.roll(rcorner[n, 1], HALF, 1), rcorner[n, 0])
            X[PAD - EDGE : PAD, :] = edges_of(rtop[n, 0], rtop[n, NB - 1], beyond)

    messages.land()

    def joined(pick):
        return jnp.concatenate([pick(t) for t in range(C)], axis=1)

    def places(pick):
        code = joined(pick).astype(jnp.int32)
        return divide(code, BC * C), remainder(code, BC)

    place_r = iota((BR, S), 0)
    place_c = iota((BC, S), 0)

    def one_hot(hit):
        return jnp.where(hit, 1.0, 0.0).astype(BF16)

    in_row, in_col = places(lambda t: msg_row[t, 1, 0:1, :])
    in_weight = joined(lambda t: msg_row[t, 1, 1:2, :])
    row_hit = place_r == in_row
    col_hot = one_hot(place_c == in_col)
    hot_own[...] = col_hot
    hi, lo = halves(cinit[...])
    seen = dot(hi, col_hot) + dot(lo, col_hot)
    at_via = jnp.sum(jnp.where(row_hit, seen, 0.0), axis=0, keepdims=True)
    for t in range(C):
        val_out[t] = at_via[:, t * per : (t + 1) * per]
    val_in[col] = val_out[col]
    values = Batch(always, always, [
        (val_out.at[lax.rem(col + d, C)], val_in.at[col], (row, lax.rem(col + d, C)))
        for d in range(1, C)
    ])

    dinv_copies = halo_send(dv, 0)

    def spread(hit, amount):
        hi, lo = halves(amount)
        zero = jnp.zeros((), BF16)
        return jnp.concatenate([jnp.where(hit, hi, zero), jnp.where(hit, lo, zero)], axis=0)

    cleak_load.wait()
    only = jnp.where(row_hit, in_weight, 0.0).astype(BF16)
    coarse_diag = 4.0 * coarse_conductance + cleak[...] + dot_t(only, col_hot)
    scale = relaxation / coarse_diag
    place = iota((BR, BC), 1)
    place_v = iota((BR, BC), 0)
    within = remainder(place, GROUP)
    group = iota((groups, BR), 0)

    def beside(volt, n, above, below, far_left, far_right):
        above = jnp.where(place_v == 0, keep(top_ok, above), pltpu.roll(volt, 1, 0))
        below = jnp.where(place_v == BR - 1, keep(bot_ok, below), pltpu.roll(volt, BR - 1, 0))
        turn[n, pl.ds(0, groups, stride=GROUP), :] = jnp.where(
            left_ok, far_left, jnp.where(group == 0, 0.0, jnp.roll(far_left, 1, 0))
        )
        turn[n, pl.ds(GROUP - 1, groups, stride=GROUP), :] = jnp.where(
            right_ok, far_right, jnp.where(group == groups - 1, 0.0, jnp.roll(far_right, -1, 0))
        )
        edge = turn[n].T
        before = jnp.where(within == 0, edge, pltpu.roll(volt, 1, 1))
        after = jnp.where(within == GROUP - 1, edge, pltpu.roll(volt, BC - 1, 1))
        return above + below + before + after

    coarse_land(coarse0, 0)
    volt = cinit[...]
    sides = beside(volt, 0, crow_top[0, 7:8, :], crow_bot[0, 0:1, :], cleft[0], cright[0])
    coarse[0] = volt + scale * (coarse_conductance * sides - coarse_diag * volt)
    coarse[1] = scale
    coarse[2] = coarse_diag
    coarse_later = []
    for n in range(2):
        seams(coarse[n], n + 1)
        coarse_later.append(coarse_send(coarse.at[n], n + 1))

    def quiet(ref, shape):
        def body():
            for t in range(C):
                ref[t] = jnp.zeros(shape, F32)
        return body

    messages_down.land(quiet(msg_ud.at[0], (2, per)))
    messages_up.land(quiet(msg_ud.at[1], (2, per)))
    left_row, left_col = places(lambda t: msg_row[t, 0, 0:1, :])
    right_row, right_col = places(lambda t: msg_row[t, 2, 0:1, :])
    above_row, above_col = places(lambda t: msg_ud[0, t, 0:1, :])
    below_row, below_col = places(lambda t: msg_ud[1, t, 0:1, :])
    hot_left[...] = one_hot(place_r == left_row)
    hot_right[...] = one_hot(place_r == right_row)
    hot_up[...] = one_hot(place_c == above_col)
    hot_down[...] = one_hot(place_c == below_col)

    def edge_copy(F, X, size):
        X[...] = edges_of(F[0:TR, :], F[(NB - 1) * size : (NB - 1) * size + TR, :], None)

    edge_copy(D, Dq, TR)
    halo_land(dv, dvq, 0, dinv_copies)

    for copy in amp_loads:
        copy.wait()
    values.land()
    drops = weight * joined(lambda o: val_in[o])
    drop_hi, drop_lo = halves(drops)
    half_step = 128 if TR % 128 == 0 else step

    def inject(i, carry):
        at = pl.ds(pl.multiple_of(i * half_step, half_step), half_step)
        hot = row_hot[at, :]
        added = dot(hot * drop_hi, Bt[...]) + dot(hot * drop_lo, Bt[...])
        for b in range(NB):
            inner = pl.ds(pl.multiple_of(b * EXT + PAD + i * half_step, 8), half_step)
            own = pl.ds(pl.multiple_of(b * TR + i * half_step, 8), half_step)
            value = amp[b, at, :] * mask[b, at, :].astype(F32) + added[:, b * LANES : (b + 1) * LANES]
            rhs[own, :] = value
            V[0, inner, :] = value * dv[inner, :]
        return carry

    lax.fori_loop(0, TR // half_step, inject, 0)
    first_copies = halo_send(V.at[0], 1)
    edge_copy(rhs, rhsq, TR)

    def stencil(k, start, size):
        place = wide(size)
        mids = [V[k, pl.ds(b * EXT + start, size), :] for b in range(NB)]
        lefts = [pltpu.roll(m, 1, 1) for m in mids]
        rights = [pltpu.roll(m, LANES - 1, 1) for m in mids]
        out = []
        for b in range(NB):
            tall = V[k, pl.ds(b * EXT + start - 1, size), :] + V[k, pl.ds(b * EXT + start + 1, size), :]
            before = jnp.where(place == 0, lefts[b - 1], lefts[b])
            after = jnp.where(place == LANES - 1, rights[(b + 1) % NB], rights[b])
            out.append(tall + (before + after))
        return mids, out

    def inward(b, value):
        place = wide(value.shape[0])
        if b == 0:
            value = jnp.where(place >= EDGE, value, 0.0)
        if b == NB - 1:
            value = jnp.where(place < LANES - EDGE, value, 0.0)
        return value

    def advance(k, start, size, totals):
        mids, near = stencil(k, start, size)
        totals = None if totals is None else list(totals)
        for b in range(NB):
            at = pl.ds(b * EXT + start, size)
            own = pl.ds(b * TR + start - PAD, size)
            if k < ITERS - 1:
                fresh = dv[at, :] * near[b]
                if k:
                    fresh = (fresh + fresh) - V[k - 1, at, :]
                V[k + 1, at, :] = fresh
                if totals is None:
                    continue
                if k == 0:
                    right_side = rhs[own, :]
                    applied = inward(b, right_side - near[b])
                    R0[own, :] = applied
                    totals[0] = totals[0] + fold(right_side * mids[b])
                    totals[1] = totals[1] + fold(applied * mids[b])
                    totals[2] = totals[2] + fold(applied * fresh)
                else:
                    totals[0] = totals[0] + fold(R0[own, :] * fresh)
            elif totals is not None:
                applied = inward(b, D[own, :] * mids[b] - near[b])
                totals[ITERS - 2] = totals[ITERS - 2] + fold(applied * mids[b])
                for j in range(1, ITERS - 1):
                    totals[j - 1] = totals[j - 1] + fold(applied * V[j, at, :])
        return None if totals is None else tuple(totals)

    def blank(n):
        return tuple(jnp.zeros((8, LANES), F32) for _ in range(n))

    kept = [3] + [1] * (ITERS - 2) + [ITERS - 1]
    chunk = 16
    sums = []
    for k in range(ITERS):
        if k < ITERS - 1:
            advance(k, PAD, EDGE, None)
            advance(k, PAD + TR - EDGE, EDGE, None)

        def body(i, carry, k=k):
            return advance(k, PAD + EDGE + i * chunk, chunk, carry)

        sums.append(lax.fori_loop(0, (TR - 2 * EDGE) // chunk, body, blank(kept[k])))

    halo_land(V.at[0], Q.at[0], 1, first_copies)
    for k in range(ITERS):
        if k < ITERS - 1:
            advance(k, PAD - EDGE, EDGE, None)
            advance(k, PAD + TR, EDGE, None)
        sums[k] = advance(k, PAD, EDGE, sums[k])
        sums[k] = advance(k, PAD + TR - EDGE, EDGE, sums[k])

    def rim(value):
        place = wide(value.shape[0])
        ours = (place < EDGE) | ((place >= HALF - EDGE) & (place < HALF))
        return jnp.where(ours, value, 0.0)

    def advance_edge(k, start, size, totals):
        mid = Q[k, pl.ds(start, size), :]
        near = Q[k, pl.ds(start - 1, size), :] + Q[k, pl.ds(start + 1, size), :]
        near = near + (pltpu.roll(mid, 1, 1) + pltpu.roll(mid, LANES - 1, 1))
        at = pl.ds(start, size)
        own = pl.ds(start - PAD, size)
        totals = None if totals is None else list(totals)
        if k < ITERS - 1:
            fresh = dvq[at, :] * near
            if k:
                fresh = (fresh + fresh) - Q[k - 1, at, :]
            Q[k + 1, at, :] = fresh
            if totals is not None:
                if k == 0:
                    applied = rim(rhsq[own, :] - near)
                    rhsq[own, :] = applied
                    totals[1] = totals[1] + fold(applied * mid)
                    totals[2] = totals[2] + fold(applied * fresh)
                else:
                    totals[0] = totals[0] + fold(rhsq[own, :] * fresh)
        elif totals is not None:
            applied = rim(Dq[own, :] * mid - near)
            totals[ITERS - 2] = totals[ITERS - 2] + fold(applied * mid)
            for j in range(1, ITERS - 1):
                totals[j - 1] = totals[j - 1] + fold(applied * Q[j, at, :])
        return None if totals is None else tuple(totals)

    edge_chunk = 64
    for k in range(ITERS):
        if k < ITERS - 1:
            advance_edge(k, PAD - EDGE, EDGE, None)
            advance_edge(k, PAD + TR, EDGE, None)

        def body(i, carry, k=k):
            return advance_edge(k, PAD + i * edge_chunk, edge_chunk, carry)

        sums[k] = lax.fori_loop(0, TR // edge_chunk, body, sums[k])

    flat = [total for part in sums for total in part]
    tile = jnp.concatenate([jnp.sum(total, axis=0, keepdims=True) for total in flat], axis=0)
    sub = iota((8, LANES), 0)
    number = len(flat)
    tile = jnp.sum(tile, axis=1, keepdims=True)
    red_out[...] = jnp.sum(jnp.where(sub == lane_row, tile, 0.0), axis=0, keepdims=True)
    me = row * C + col
    red_in[me] = red_out[...]
    reductions = Batch(always, always, [
        (red_out, red_in.at[me], (lax.rem(row + e, R), lax.rem(col + d, C)))
        for e in reversed(range(R)) for d in reversed(range(C)) if e or d
    ])

    def patch(i, carry):
        for k in range(1, ITERS):
            at = pl.ds(PAD + i * edge_chunk, edge_chunk)
            far = pl.ds(last + PAD + i * edge_chunk, edge_chunk)
            edge = Q[k, at, :]
            place = wide(edge_chunk)
            V[k, at, :] = jnp.where(place < EDGE, edge, V[k, at, :])
            V[k, far, :] = jnp.where(place >= LANES - EDGE, pltpu.roll(edge, HALF, 1), V[k, far, :])
        return carry

    lax.fori_loop(0, TR // edge_chunk, patch, 0)
    spot_copy.wait()
    unroll = 8

    def pick(i, carry):
        for n in range(unroll):
            s = i * unroll + n
            where = spot[0, s]
            for k in range(ITERS):
                picked[k, pl.ds(s, 1), :] = V[k, pl.ds(where, 1), :]
        return carry

    lax.fori_loop(0, S // unroll, pick, 0)
    diag_hit = iota((per, LANES), 0) == iota((per, LANES), 1)

    for o in range(C):
        part = slice(o * per, (o + 1) * per)
        hot = lane_hot[part, :]
        for k in range(ITERS):
            value = jnp.sum(picked[k, part, :] * hot, axis=1, keepdims=True)
            seen_out[o + 1, k : k + 1, :] = jnp.sum(jnp.where(diag_hit, value, 0.0), axis=0, keepdims=True)
    seen_out[0] = seen_out[C]
    seen_out[C + 1] = seen_out[1]
    seen_row[col] = seen_out[pl.ds(col, 3)]
    seen_side = Batch(always, always, [
        (seen_out.at[pl.ds(lax.rem(col + d, C), 3)], seen_row.at[col], (row, lax.rem(col + d, C)))
        for d in range(1, C)
    ])
    seen_up = Batch(top_ok, bot_ok, [
        (seen_out.at[lax.rem(col + d, C) + 1], seen_ud.at[1, col], (up, lax.rem(col + d, C)))
        for d in range(C)
    ])
    seen_down = Batch(bot_ok, top_ok, [
        (seen_out.at[lax.rem(col + d, C) + 1], seen_ud.at[0, col], (down, lax.rem(col + d, C)))
        for d in range(C)
    ])

    reductions.land()
    parts = [red_in[n] for n in range(R * C)]
    while len(parts) > 1:
        parts = [sum(parts[n : n + 2][1:], parts[n]) for n in range(0, len(parts), 2)]
    total = jnp.broadcast_to(parts[0], (8, LANES))
    total = jnp.sum(jnp.where(sub == lane_row, total, 0.0), axis=1, keepdims=True)
    scalar = [total[n : n + 1, :] for n in range(number)]
    energy = [scalar[1], scalar[2]] + scalar[3 : 3 + ITERS - 2]
    high = scalar[3 + ITERS - 2 :]
    for j in range(1, ITERS):
        energy.append(2.0 * high[j - 1] - energy[ITERS - 1 - j])
    moment = [scalar[0], scalar[0] - energy[0]]
    for n in range(2, ITERS):
        moment.append(2.0 * (moment[n - 1] - energy[n - 1]) - moment[n - 2])
    matrix = [[None] * (ITERS + 1) for _ in range(ITERS)]
    for j in range(ITERS):
        for k in range(j + 1):
            matrix[j][k] = matrix[k][j] = 0.5 * (energy[j + k] + energy[j - k])
        matrix[j][ITERS] = moment[j]
    for i in range(ITERS):
        inverse = 1.0 / matrix[i][i]
        for k in range(i + 1, ITERS + 1):
            matrix[i][k] = matrix[i][k] * inverse
        for j in range(i + 1, ITERS):
            for k in range(i + 1, ITERS + 1):
                matrix[j][k] = matrix[j][k] - matrix[j][i] * matrix[i][k]
    coef = [None] * ITERS
    for i in reversed(range(ITERS)):
        coef[i] = matrix[i][ITERS]
        for k in range(i + 1, ITERS):
            coef[i] = coef[i] - matrix[i][k] * coef[k]
    coef = [jnp.broadcast_to(c, (1, LANES)) for c in coef]

    def finish(i, carry):
        at = pl.ds(pl.multiple_of(i * step, step), step)
        for b in range(NB):
            inner = pl.ds(pl.multiple_of(b * EXT + PAD + i * step, 8), step)
            value = coef[0] * V[0, inner, :]
            for k in range(1, ITERS):
                value = value + coef[k] * V[k, inner, :]
            x_out[at, b * LANES : (b + 1) * LANES] = value
        return carry

    lax.fori_loop(0, TR // step, finish, 0)

    for n in range(2):
        coarse_land(coarse_later[n], n + 1)
    seen_side.land()
    seen_down.land(quiet(seen_ud.at[0], (ITERS, per)))
    seen_up.land(quiet(seen_ud.at[1], (ITERS, per)))

    def amount(value, weights):
        def one(t):
            seen = value(t)
            total = coef[0] * seen[0:1, :]
            for k in range(1, ITERS):
                total = total + coef[k] * seen[k : k + 1, :]
            return total * weights(t)
        return joined(one)

    def gathered(hit, value, weights, hot):
        out = dot_t(spread(hit, amount(value, weights)), hot)
        return out[: out.shape[0] // 2] + out[out.shape[0] // 2 :]

    place_g = iota((groups, S), 0) * GROUP
    one_row = iota((8, S), 0) == 0
    own_row, own_col = places(lambda t: msg_row[t, 1, 0:1, :])
    sources = gathered(
        place_r == own_row, lambda t: seen_row[t, 1], lambda t: msg_row[t, 1, 1:2, :], hot_own[...]
    )
    from_left = gathered(
        place_g + (GROUP - 1) == left_col, lambda t: seen_row[t, 0], lambda t: msg_row[t, 0, 1:2, :],
        hot_left[...],
    )
    from_right = gathered(
        place_g == right_col, lambda t: seen_row[t, 2], lambda t: msg_row[t, 2, 1:2, :], hot_right[...]
    )
    from_above = gathered(
        one_row & (above_row == BR - 1), lambda t: seen_ud[0, t], lambda t: msg_ud[0, t, 1:2, :], hot_up[...]
    )
    from_below = gathered(
        one_row & (below_row == 0), lambda t: seen_ud[1, t], lambda t: msg_ud[1, t, 1:2, :], hot_down[...]
    )
    scale = coarse[1]
    volt = coarse[0] + scale * sources
    sides = beside(
        volt, 0,
        crow_top[1, 7:8, :] + crow_top[2, 7:8, :] * from_above[0:1, :],
        crow_bot[1, 0:1, :] + crow_bot[2, 0:1, :] * from_below[0:1, :],
        cleft[1] + cleft[2] * from_left,
        cright[1] + cright[2] * from_right,
    )
    c_out[...] = volt + scale * (sources + coarse_conductance * sides - coarse[2] * volt)
    for batch in pending:
        batch.leave()


def per_device(R, C, load_amp, load_mask, leak, coarse_leak, coarse_init, via_fine, via_coarse, via_count):
    TR, TC = leak.shape
    BR, BC = coarse_leak.shape
    S = via_fine.shape[1]
    per = S // C
    NB = TC // LANES
    EXT = TR + 2 * PAD
    groups = BC // GROUP
    copies = 3 * (C - 1) + 4 * C + 2 * (2 + 2 * (2 + NB)) + 12 + R * C - 1
    vmem = pl.BlockSpec(memory_space=pltpu.VMEM)
    return pl.pallas_call(
        functools.partial(kernel, R, C),
        out_shape=(pltpu.VMEM((TR, TC), F32), pltpu.VMEM((BR, BC), F32)),
        in_specs=[pl.BlockSpec(memory_space=pltpu.HBM)] * 8,
        out_specs=(vmem, vmem),
        scratch_shapes=[
            pltpu.VMEM((NB, TR, LANES), F32), pltpu.VMEM((NB, TR, LANES), jnp.int32),
            pltpu.VMEM((NB, TR, LANES), F32),
            pltpu.VMEM((BR, BC), F32), pltpu.VMEM((BR, BC), F32),
            pltpu.VMEM((1, S), jnp.int32), pltpu.VMEM((1, S), jnp.int32),
            pltpu.SMEM((1, C), jnp.int32), pltpu.SemaphoreType.DMA((3 * NB + 6,)),
            pltpu.VMEM((C + 2, 2, per), F32), pltpu.VMEM((C, 3, 2, per), F32), pltpu.VMEM((2, C, 2, per), F32),
            pltpu.VMEM((C, 1, per), F32), pltpu.VMEM((C, 1, per), F32),
            pltpu.VMEM((C + 2, ITERS, per), F32), pltpu.VMEM((C, 3, ITERS, per), F32),
            pltpu.VMEM((2, C, ITERS, per), F32),
            pltpu.VMEM((1, S), jnp.int32), pltpu.SMEM((1, S), jnp.int32),
            pltpu.VMEM((ITERS, S, LANES), F32), pltpu.VMEM((S, LANES), F32),
            pltpu.VMEM((TR, S), BF16),
            pltpu.VMEM((S, TC), BF16),
            pltpu.VMEM((NB * EXT, LANES), F32),
            pltpu.VMEM((NB * TR, LANES), F32),
            pltpu.VMEM((EXT, LANES), F32),
            pltpu.VMEM((TR, LANES), F32),
            pltpu.VMEM((ITERS, NB * EXT, LANES), F32),
            pltpu.VMEM((ITERS, EXT, LANES), F32),
            pltpu.VMEM((NB * TR, LANES), F32),
            pltpu.VMEM((NB * TR, LANES), F32),
            pltpu.VMEM((TR, LANES), F32),
            pltpu.VMEM((2, TR, LANES), F32),
            pltpu.VMEM((2, LANES, TR), F32),
            pltpu.VMEM((2, LANES, TR), F32),
            pltpu.VMEM((2, NB, EDGE, LANES), F32),
            pltpu.VMEM((2, NB, EDGE, LANES), F32),
            pltpu.VMEM((2, 4, EDGE, LANES), F32),
            pltpu.VMEM((1, LANES), F32), pltpu.VMEM((R * C, 1, LANES), F32),
            pltpu.VMEM((BC, S), BF16), pltpu.VMEM((BR, S), BF16), pltpu.VMEM((BR, S), BF16),
            pltpu.VMEM((BC, S), BF16), pltpu.VMEM((BC, S), BF16),
            pltpu.VMEM((3, BR, BC), F32),
            pltpu.VMEM((3, BC, BR), F32), pltpu.VMEM((3, 2, groups, BR), F32),
            pltpu.VMEM((3, 8, BC), F32), pltpu.VMEM((3, 8, BC), F32),
            pltpu.VMEM((3, groups, BR), F32), pltpu.VMEM((3, groups, BR), F32),
            pltpu.SemaphoreType.DMA((copies,)),
            pltpu.SemaphoreType.DMA((copies,)),
        ],
        compiler_params=pltpu.CompilerParams(
            collective_id=0, has_side_effects=True, vmem_limit_bytes=58000 * 1024
        ),
    )(load_amp, load_mask, leak, coarse_leak, coarse_init, via_fine, via_coarse, via_count)


def solution(mesh):
    spec = P("row", "col")
    return jax.shard_map(
        functools.partial(per_device, mesh.shape["row"], mesh.shape["col"]),
        mesh=mesh, in_specs=(spec,) * 8, out_specs=(spec, spec), check_vma=False,
    )
```

```python
import functools
import jax
import jax.numpy as jnp
from jax import lax
from jax.experimental import pallas as pl
from jax.experimental.pallas import tpu as pltpu
from jax.sharding import PartitionSpec as P

GROUP = 16
ITERS = 4
LANES = 128
PAD = 16
EDGE = 8
HALF = LANES // 2
QUARTER = LANES // 4

via_conductance = 2.0
coarse_conductance = 4.0
relaxation = 0.8

F32 = jnp.float32
BF16 = jnp.bfloat16
MESH = pl.DeviceIdType.MESH


def divide(value, by):
    if by & (by - 1) == 0:
        return lax.shift_right_logical(value, by.bit_length() - 1)
    return value // by


def remainder(value, by):
    if by & (by - 1) == 0:
        return value & (by - 1)
    return value % by


def halves(value):
    high = value.astype(BF16).astype(F32)
    return high.astype(BF16), (value - high).astype(BF16)


def dot(a, b):
    return jnp.dot(a, b, preferred_element_type=F32)


def dot_t(a, b):
    return lax.dot_general(a, b, (((1,), (1,)), ((), ())), preferred_element_type=F32)


def fold(value):
    total = value[0:8]
    for n in range(1, value.shape[0] // 8):
        total = total + value[n * 8 : (n + 1) * 8]
    return total


def iota(shape, dim):
    return lax.broadcasted_iota(jnp.int32, shape, dim)


def kernel(
    R, C,
    amp_in, mask_in, leak_in, cleak_in, cinit_in, vf_in, vc_in, cnt_in,
    x_out, c_out,
    amp, mask, leak, cleak, cinit, vf, vc, cnt, load_sem,
    msg_out, msg_row, msg_ud, val_out, val_in, seen_out, seen_row, seen_ud,
    spot_v, spot, woven, picked, lane_hot,
    row_hot, Bt, dv, D, dvq, Dq, V, Q, R0, rhs, rhsq,
    E, ET, H, rtop, rbot, rcorner,
    red_out, red_in,
    hot_own, hot_left, hot_right, hot_up, hot_down,
    coarse, turn, seam_out, crow_top, crow_bot, cleft, cright,
    send_sem, recv_sem,
):
    row, col = lax.axis_index("row"), lax.axis_index("col")
    TR, TC = leak_in.shape
    NB = TC // LANES
    EXT = TR + 2 * PAD
    BR, BC = cleak.shape
    S = vf.shape[1]
    per = S // C
    groups = BC // GROUP

    def cut(b):
        return pl.ds(b * LANES, LANES)

    loads = []

    def load(source, target):
        copy = pltpu.make_async_copy(source, target, load_sem.at[len(loads)])
        copy.start()
        loads.append(copy)
        return copy

    small = [load(cnt_in, cnt), load(vc_in, vc), load(vf_in, vf)]
    cinit_load = load(cinit_in, cinit)
    leak_loads = [load(leak_in.at[:, cut(b)], leak.at[b]) for b in range(NB)]
    cleak_load = load(cleak_in, cleak)
    amp_loads = [load(amp_in.at[:, cut(b)], amp.at[b]) for b in range(NB)]
    amp_loads += [load(mask_in.at[:, cut(b)], mask.at[b]) for b in range(NB)]

    up, down = lax.rem(row + R - 1, R), lax.rem(row + 1, R)
    left, right = lax.rem(col + C - 1, C), lax.rem(col + 1, C)
    top_ok, bot_ok = row > 0, row < R - 1
    left_ok, right_ok = col > 0, col < C - 1
    always = None

    barrier = pltpu.get_barrier_semaphore()

    def greet(r, c):
        pl.semaphore_signal(barrier, inc=1, device_id=(r, c), device_id_type=MESH)

    for d in range(1, C):
        greet(row, lax.rem(col + d, C))
    near_rows = R <= 4
    if near_rows:

        @pl.when(top_ok)
        def _():
            for d in range(C):
                greet(up, lax.rem(col + d, C))

        @pl.when(bot_ok)
        def _():
            for d in range(C):
                greet(down, lax.rem(col + d, C))
    else:
        for e in range(1, R):
            for d in range(C):
                greet(lax.rem(row + e, R), lax.rem(col + d, C))

    def welcome():
        if near_rows:
            rows = jnp.where(top_ok, 1, 0) + jnp.where(bot_ok, 1, 0)
            pl.semaphore_wait(barrier, C - 1 + C * rows)
        else:
            pl.semaphore_wait(barrier, R * C - 1)

    count = [0]
    pending = []

    def under(ok, body):
        if ok is always:
            body()
        else:
            pl.when(ok)(body)

    class Batch:
        def __init__(self, ok, heard, specs):
            self.ok, self.heard = ok, heard
            self.copies = []
            for src, dst, device in specs:
                n = count[0]
                count[0] += 1
                self.copies.append(pltpu.make_async_remote_copy(
                    src_ref=src, dst_ref=dst, send_sem=send_sem.at[n], recv_sem=recv_sem.at[n],
                    device_id=device, device_id_type=MESH,
                ))
            pending.append(self)

            def start():
                for copy in self.copies:
                    copy.start()

            under(ok, start)

        def land(self, otherwise=None):
            def wait():
                for copy in self.copies:
                    copy.wait_recv()

            under(self.heard, wait)
            if self.heard is not always and otherwise is not None:
                pl.when(jnp.logical_not(self.heard))(otherwise)

        def leave(self):
            def wait():
                for copy in self.copies:
                    copy.wait_send()

            under(self.ok, wait)

    for copy in small:
        copy.wait()
    lane = iota((1, per), 1)
    weight = jnp.concatenate(
        [jnp.where(lane < cnt[0, o], via_conductance, 0.0).astype(F32) for o in range(C)], axis=1
    )
    node = vc[...].astype(F32)
    for o in [-1] + list(range(C)) + [C]:
        part = slice((o % C) * per, (o % C + 1) * per)
        msg_out[o + 1, 0:1, :] = node[:, part]
        msg_out[o + 1, 1:2, :] = weight[:, part]
    msg_row[col] = msg_out[pl.ds(col, 3)]
    fine = vf[...]
    fine_row = divide(fine, TC)
    fine_col = remainder(fine, TC)
    spot_v[...] = (divide(fine_col, LANES) * TR + fine_row) * ITERS
    spot_copy = pltpu.make_async_copy(spot_v, spot, load_sem.at[len(loads)])
    spot_copy.start()
    step = 64

    def build_rows(i, carry):
        at = pl.ds(pl.multiple_of(i * step, step), step)
        place = iota((step, S), 0) + i * step
        row_hot[at, :] = jnp.where(place == fine_row, 1.0, 0.0).astype(BF16)
        return carry

    lax.fori_loop(0, TR // step, build_rows, 0)

    welcome()

    messages = Batch(always, always, [
        (msg_out.at[pl.ds(lax.rem(col + d, C), 3)], msg_row.at[col], (row, lax.rem(col + d, C)))
        for d in range(1, C)
    ])

    def seams(volt, n):
        turn[n] = volt.T
        seam_out[n, 0] = turn[n, pl.ds(0, groups, stride=GROUP), :]
        seam_out[n, 1] = turn[n, pl.ds(GROUP - 1, groups, stride=GROUP), :]

    def coarse_send(ref, n):
        return [
            Batch(top_ok, bot_ok, [(ref.at[pl.ds(0, 8)], crow_bot.at[n], (up, col))]),
            Batch(bot_ok, top_ok, [(ref.at[pl.ds(BR - 8, 8)], crow_top.at[n], (down, col))]),
            Batch(always, always, [
                (seam_out.at[n, 0], cright.at[n], (row, left)),
                (seam_out.at[n, 1], cleft.at[n], (row, right)),
            ]),
        ]

    def coarse_land(batches, n):
        def no_below():
            crow_bot[n] = jnp.zeros((8, BC), F32)

        def no_above():
            crow_top[n] = jnp.zeros((8, BC), F32)

        batches[0].land(no_below)
        batches[1].land(no_above)
        batches[2].land()

    cinit_load.wait()
    seams(cinit[...], 0)
    coarse0 = coarse_send(cinit, 0)
    messages_up = Batch(top_ok, bot_ok, [
        (msg_out.at[lax.rem(col + d, C) + 1], msg_ud.at[1, col], (up, lax.rem(col + d, C)))
        for d in range(C)
    ])
    messages_down = Batch(bot_ok, top_ok, [
        (msg_out.at[lax.rem(col + d, C) + 1], msg_ud.at[0, col], (down, lax.rem(col + d, C)))
        for d in range(C)
    ])

    lanes = iota((per, LANES), 1).astype(F32)
    for o in range(C):
        part = slice(o * per, (o + 1) * per)
        turned = jnp.broadcast_to(fine_col[:, part].astype(F32), (LANES, per)).T
        near = turned
        total = jnp.zeros((per, LANES), F32)
        for b in range(NB):
            hot = jnp.where(turned == lanes + b * LANES, 1.0, 0.0)
            Bt[part, b * LANES : (b + 1) * LANES] = hot.astype(BF16)
            total = total + hot
        lane_hot[part, :] = total

    zero_pad = jnp.zeros((8, LANES), F32)
    for n in range(ITERS):
        for b in range(NB):
            V[n, b * EXT : b * EXT + 8, :] = zero_pad
            V[n, (b + 1) * EXT - 8 : (b + 1) * EXT, :] = zero_pad
        for b in range(NB if n == 0 else 0):
            V[n, b * EXT + 8 : b * EXT + 16, :] = zero_pad
            V[n, (b + 1) * EXT - 16 : (b + 1) * EXT - 8, :] = zero_pad
        Q[n, 0:8, :] = zero_pad
        Q[n, EXT - 8 : EXT, :] = zero_pad
    for n in range(1, ITERS):
        for b in range(NB):
            V[n, b * EXT + 8 : b * EXT + 16, :] = zero_pad
            V[n, (b + 1) * EXT - 16 : (b + 1) * EXT - 8, :] = zero_pad

    for copy in leak_loads:
        copy.wait()
    wide_step = 256 if TR % 256 == 0 else step
    weight_low = weight.astype(BF16)

    def diagonal(i, carry):
        at = pl.ds(pl.multiple_of(i * wide_step, wide_step), wide_step)
        sums = dot(row_hot[at, :] * weight_low, Bt[...])
        for b in range(NB):
            inner = pl.ds(pl.multiple_of(b * EXT + PAD + i * wide_step, 8), wide_step)
            own = pl.ds(pl.multiple_of(b * TR + i * wide_step, 8), wide_step)
            value = 4.0 + leak[b, at, :] + sums[:, b * LANES : (b + 1) * LANES]
            D[own, :] = value
            dv[inner, :] = 1.0 / value
        return carry

    lax.fori_loop(0, TR // wide_step, diagonal, 0)

    lane_row = iota((8, LANES), 1)

    def wide(rows):
        return iota((rows, LANES), 1)

    def keep(ok, value):
        return value * jnp.where(ok, 1.0, 0.0).astype(F32)

    last = (NB - 1) * EXT

    def halo_send(F, n):
        edge = jnp.where(wide(TR) < HALF, F[PAD : PAD + TR, :], F[last + PAD : last + PAD + TR, :])
        E[n] = edge
        ET[n] = edge.T
        ends = [(PAD, up), (PAD + TR - EDGE, down)]
        sides = Batch(always, always, [
            (ET.at[n, pl.ds(0, EDGE)], H.at[n, pl.ds(HALF, EDGE)], (row, left)),
            (ET.at[n, pl.ds(LANES - EDGE, EDGE)], H.at[n, pl.ds(LANES - EDGE, EDGE)], (row, right)),
        ])
        above = Batch(top_ok, bot_ok, [
            (E.at[n, pl.ds(0, EDGE)], rcorner.at[n, 3], (up, left)),
            (E.at[n, pl.ds(0, EDGE)], rcorner.at[n, 2], (up, right)),
        ] + [
            (F.at[pl.ds(b * EXT + PAD, EDGE)], rbot.at[n, b], (up, col)) for b in range(NB)
        ])
        below = Batch(bot_ok, top_ok, [
            (E.at[n, pl.ds(TR - EDGE, EDGE)], rcorner.at[n, 1], (down, left)),
            (E.at[n, pl.ds(TR - EDGE, EDGE)], rcorner.at[n, 0], (down, right)),
        ] + [
            (F.at[pl.ds(b * EXT + PAD + TR - EDGE, EDGE)], rtop.at[n, b], (down, col)) for b in range(NB)
        ])
        return sides, above, below

    def edges_of(first, final, beyond):
        rows = first.shape[0]
        place = wide(rows)
        own = jnp.where(place < QUARTER, first, pltpu.roll(final, HALF, 1))
        if beyond is None:
            return own
        return jnp.where(place < HALF, own, beyond)

    def outer(right_side, left_side):
        place = wide(right_side.shape[0])
        right_side = jnp.where((place < HALF + EDGE) & right_ok, right_side, 0.0)
        return jnp.where((place >= LANES - EDGE) & left_ok, left_side, right_side)

    def halo_land(F, X, n, batches):
        sides, above, below = batches
        sides.land()
        side = H[n].T
        X[PAD : PAD + TR, :] = edges_of(
            F[PAD : PAD + TR, :], F[last + PAD : last + PAD + TR, :], outer(side, side)
        )

        def no_below():
            for b in range(NB):
                F[b * EXT + PAD + TR : b * EXT + PAD + TR + EDGE, :] = zero_pad
            X[PAD + TR : PAD + TR + EDGE, :] = zero_pad

        def no_above():
            for b in range(NB):
                F[b * EXT + PAD - EDGE : b * EXT + PAD, :] = zero_pad
            X[PAD - EDGE : PAD, :] = zero_pad

        above.land(no_below)
        below.land(no_above)

        @pl.when(bot_ok)
        def _():
            for b in range(NB):
                F[b * EXT + PAD + TR : b * EXT + PAD + TR + EDGE, :] = rbot[n, b]
            beyond = outer(pltpu.roll(rcorner[n, 3], HALF, 1), rcorner[n, 2])
            X[PAD + TR : PAD + TR + EDGE, :] = edges_of(rbot[n, 0], rbot[n, NB - 1], beyond)

        @pl.when(top_ok)
        def _():
            for b in range(NB):
                F[b * EXT + PAD - EDGE : b * EXT + PAD, :] = rtop[n, b]
            beyond = outer(pltpu.roll(rcorner[n, 1], HALF, 1), rcorner[n, 0])
            X[PAD - EDGE : PAD, :] = edges_of(rtop[n, 0], rtop[n, NB - 1], beyond)

    dinv_copies = halo_send(dv, 0)

    messages.land()

    def joined(pick):
        return jnp.concatenate([pick(t) for t in range(C)], axis=1)

    def places(pick):
        code = joined(pick).astype(jnp.int32)
        return divide(code, BC * C), remainder(code, BC)

    place_r = iota((BR, S), 0)
    place_c = iota((BC, S), 0)

    def one_hot(hit):
        return jnp.where(hit, 1.0, 0.0).astype(BF16)

    in_row, in_col = places(lambda t: msg_row[t, 1, 0:1, :])
    in_weight = joined(lambda t: msg_row[t, 1, 1:2, :])
    row_hit = place_r == in_row
    col_hot = one_hot(place_c == in_col)
    hot_own[...] = col_hot
    hi, lo = halves(cinit[...])
    seen = dot(hi, col_hot) + dot(lo, col_hot)
    at_via = jnp.sum(jnp.where(row_hit, seen, 0.0), axis=0, keepdims=True)
    for t in range(C):
        val_out[t] = at_via[:, t * per : (t + 1) * per]
    val_in[col] = val_out[col]
    values = Batch(always, always, [
        (val_out.at[lax.rem(col + d, C)], val_in.at[col], (row, lax.rem(col + d, C)))
        for d in range(1, C)
    ])

    def spread(hit, amount):
        hi, lo = halves(amount)
        zero = jnp.zeros((), BF16)
        return jnp.concatenate([jnp.where(hit, hi, zero), jnp.where(hit, lo, zero)], axis=0)

    cleak_load.wait()
    only = jnp.where(row_hit, in_weight, 0.0).astype(BF16)
    coarse_diag = 4.0 * coarse_conductance + cleak[...] + dot_t(only, col_hot)
    scale = relaxation / coarse_diag
    place = iota((BR, BC), 1)
    place_v = iota((BR, BC), 0)
    within = remainder(place, GROUP)
    group = iota((groups, BR), 0)

    def beside(volt, n, above, below, far_left, far_right):
        above = jnp.where(place_v == 0, keep(top_ok, above), pltpu.roll(volt, 1, 0))
        below = jnp.where(place_v == BR - 1, keep(bot_ok, below), pltpu.roll(volt, BR - 1, 0))
        turn[n, pl.ds(0, groups, stride=GROUP), :] = jnp.where(
            left_ok, far_left, jnp.where(group == 0, 0.0, jnp.roll(far_left, 1, 0))
        )
        turn[n, pl.ds(GROUP - 1, groups, stride=GROUP), :] = jnp.where(
            right_ok, far_right, jnp.where(group == groups - 1, 0.0, jnp.roll(far_right, -1, 0))
        )
        edge = turn[n].T
        before = jnp.where(within == 0, edge, pltpu.roll(volt, 1, 1))
        after = jnp.where(within == GROUP - 1, edge, pltpu.roll(volt, BC - 1, 1))
        return above + below + before + after

    coarse_land(coarse0, 0)
    volt = cinit[...]
    sides = beside(volt, 0, crow_top[0, 7:8, :], crow_bot[0, 0:1, :], cleft[0], cright[0])
    coarse[0] = volt + scale * (coarse_conductance * sides - coarse_diag * volt)
    coarse[1] = scale
    coarse[2] = coarse_diag
    coarse_later = []
    for n in range(2):
        seams(coarse[n], n + 1)
        coarse_later.append(coarse_send(coarse.at[n], n + 1))

    def quiet(ref, shape):
        def body():
            for t in range(C):
                ref[t] = jnp.zeros(shape, F32)
        return body

    messages_down.land(quiet(msg_ud.at[0], (2, per)))
    messages_up.land(quiet(msg_ud.at[1], (2, per)))
    left_row, left_col = places(lambda t: msg_row[t, 0, 0:1, :])
    right_row, right_col = places(lambda t: msg_row[t, 2, 0:1, :])
    above_row, above_col = places(lambda t: msg_ud[0, t, 0:1, :])
    below_row, below_col = places(lambda t: msg_ud[1, t, 0:1, :])
    hot_left[...] = one_hot(place_r == left_row)
    hot_right[...] = one_hot(place_r == right_row)
    hot_up[...] = one_hot(place_c == above_col)
    hot_down[...] = one_hot(place_c == below_col)

    def edge_copy(F, X, size):
        X[...] = edges_of(F[0:TR, :], F[(NB - 1) * size : (NB - 1) * size + TR, :], None)

    edge_copy(D, Dq, TR)
    halo_land(dv, dvq, 0, dinv_copies)

    for copy in amp_loads:
        copy.wait()
    values.land()
    drops = weight * joined(lambda o: val_in[o])
    drop_hi, drop_lo = halves(drops)
    half_step = 256 if TR % 256 == 0 else step

    def inject(i, carry):
        at = pl.ds(pl.multiple_of(i * half_step, half_step), half_step)
        hot = row_hot[at, :]
        added = dot(hot * drop_hi, Bt[...]) + dot(hot * drop_lo, Bt[...])
        for b in range(NB):
            inner = pl.ds(pl.multiple_of(b * EXT + PAD + i * half_step, 8), half_step)
            own = pl.ds(pl.multiple_of(b * TR + i * half_step, 8), half_step)
            value = amp[b, at, :] * mask[b, at, :].astype(F32) + added[:, b * LANES : (b + 1) * LANES]
            rhs[own, :] = value
            V[0, inner, :] = value * dv[inner, :]
        return carry

    lax.fori_loop(0, TR // half_step, inject, 0)
    first_copies = halo_send(V.at[0], 1)
    edge_copy(rhs, rhsq, TR)

    def stencil(k, start, size):
        place = wide(size)
        mids = [V[k, pl.ds(b * EXT + start, size), :] for b in range(NB)]
        lefts = [pltpu.roll(m, 1, 1) for m in mids]
        rights = [pltpu.roll(m, LANES - 1, 1) for m in mids]
        out = []
        for b in range(NB):
            tall = V[k, pl.ds(b * EXT + start - 1, size), :] + V[k, pl.ds(b * EXT + start + 1, size), :]
            before = jnp.where(place == 0, lefts[b - 1], lefts[b])
            after = jnp.where(place == LANES - 1, rights[(b + 1) % NB], rights[b])
            out.append(tall + (before + after))
        return mids, out

    def inward(b, value):
        place = wide(value.shape[0])
        if b == 0:
            value = jnp.where(place >= EDGE, value, 0.0)
        if b == NB - 1:
            value = jnp.where(place < LANES - EDGE, value, 0.0)
        return value

    def advance(k, start, size, totals):
        mids, near = stencil(k, start, size)
        totals = None if totals is None else list(totals)
        for b in range(NB):
            at = pl.ds(b * EXT + start, size)
            own = pl.ds(b * TR + start - PAD, size)
            if k < ITERS - 1:
                fresh = dv[at, :] * near[b]
                if k:
                    fresh = (fresh + fresh) - V[k - 1, at, :]
                V[k + 1, at, :] = fresh
                if totals is None:
                    continue
                if k == 0:
                    right_side = rhs[own, :]
                    applied = inward(b, right_side - near[b])
                    R0[own, :] = applied
                    totals[0] = totals[0] + fold(right_side * mids[b])
                    totals[1] = totals[1] + fold(applied * mids[b])
                    totals[2] = totals[2] + fold(applied * fresh)
                else:
                    totals[0] = totals[0] + fold(R0[own, :] * fresh)
            elif totals is not None:
                applied = inward(b, D[own, :] * mids[b] - near[b])
                totals[ITERS - 2] = totals[ITERS - 2] + fold(applied * mids[b])
                for j in range(1, ITERS - 1):
                    totals[j - 1] = totals[j - 1] + fold(applied * V[j, at, :])
        return None if totals is None else tuple(totals)

    def blank(n):
        return tuple(jnp.zeros((8, LANES), F32) for _ in range(n))

    kept = [3] + [1] * (ITERS - 2) + [ITERS - 1]
    inside = TR - 2 * EDGE
    chunk = inside // 2 if inside % 16 == 0 else inside
    sums = []
    for k in range(ITERS):
        if k < ITERS - 1:
            advance(k, PAD, EDGE, None)
            advance(k, PAD + TR - EDGE, EDGE, None)

        def body(i, carry, k=k):
            return advance(k, PAD + EDGE + i * chunk, chunk, carry)

        sums.append(lax.fori_loop(0, inside // chunk, body, blank(kept[k])))

    halo_land(V.at[0], Q.at[0], 1, first_copies)
    for k in range(ITERS):
        if k < ITERS - 1:
            advance(k, PAD - EDGE, EDGE, None)
            advance(k, PAD + TR, EDGE, None)
        sums[k] = advance(k, PAD, EDGE, sums[k])
        sums[k] = advance(k, PAD + TR - EDGE, EDGE, sums[k])

    def rim(value):
        place = wide(value.shape[0])
        ours = (place < EDGE) | ((place >= HALF - EDGE) & (place < HALF))
        return jnp.where(ours, value, 0.0)

    def advance_edge(k, start, size, totals):
        mid = Q[k, pl.ds(start, size), :]
        near = Q[k, pl.ds(start - 1, size), :] + Q[k, pl.ds(start + 1, size), :]
        near = near + (pltpu.roll(mid, 1, 1) + pltpu.roll(mid, LANES - 1, 1))
        at = pl.ds(start, size)
        own = pl.ds(start - PAD, size)
        totals = None if totals is None else list(totals)
        if k < ITERS - 1:
            fresh = dvq[at, :] * near
            if k:
                fresh = (fresh + fresh) - Q[k - 1, at, :]
            Q[k + 1, at, :] = fresh
            if totals is not None:
                if k == 0:
                    applied = rim(rhsq[own, :] - near)
                    rhsq[own, :] = applied
                    totals[1] = totals[1] + fold(applied * mid)
                    totals[2] = totals[2] + fold(applied * fresh)
                else:
                    totals[0] = totals[0] + fold(rhsq[own, :] * fresh)
        elif totals is not None:
            applied = rim(Dq[own, :] * mid - near)
            totals[ITERS - 2] = totals[ITERS - 2] + fold(applied * mid)
            for j in range(1, ITERS - 1):
                totals[j - 1] = totals[j - 1] + fold(applied * Q[j, at, :])
        return None if totals is None else tuple(totals)

    edge_chunk = 128 if TR % 128 == 0 else step
    for k in range(ITERS):
        if k < ITERS - 1:
            advance_edge(k, PAD - EDGE, EDGE, None)
            advance_edge(k, PAD + TR, EDGE, None)

        sums[k] = advance_edge(k, PAD, TR, sums[k])

    flat = [total for part in sums for total in part]
    tile = jnp.concatenate([jnp.sum(total, axis=0, keepdims=True) for total in flat], axis=0)
    sub = iota((8, LANES), 0)
    number = len(flat)
    tile = jnp.sum(tile, axis=1, keepdims=True)
    red_out[...] = jnp.sum(jnp.where(sub == lane_row, tile, 0.0), axis=0, keepdims=True)
    me = row * C + col
    early = len(pending)
    red_in[me] = red_out[...]
    reductions = Batch(always, always, [
        (red_out, red_in.at[me], (lax.rem(row + e, R), lax.rem(col + d, C)))
        for e in reversed(range(R)) for d in reversed(range(C)) if e or d
    ])

    def patch(i, carry):
        at = pl.ds(PAD + i * edge_chunk, edge_chunk)
        place = wide(edge_chunk)
        for b in range(NB):
            here = pl.ds(b * EXT + PAD + i * edge_chunk, edge_chunk)
            for k in range(ITERS):
                value = V[k, here, :]
                if k and b == 0:
                    value = jnp.where(place < EDGE, Q[k, at, :], value)
                if k and b == NB - 1:
                    value = jnp.where(place >= LANES - EDGE, pltpu.roll(Q[k, at, :], HALF, 1), value)
                if k and b in (0, NB - 1):
                    V[k, here, :] = value
                woven[pl.ds((b * TR + i * edge_chunk) * ITERS + k, edge_chunk, stride=ITERS), :] = value
        return carry

    lax.fori_loop(0, TR // edge_chunk, patch, 0)
    spot_copy.wait()
    unroll = 8

    def pick(i, carry):
        for n in range(unroll):
            s = i * unroll + n
            where = spot[0, s]
            picked[pl.ds(pl.multiple_of(s * ITERS, ITERS), ITERS), :] = woven[pl.ds(where, ITERS), :]
        return carry

    lax.fori_loop(0, S // unroll, pick, 0)
    diag_hit = iota((per, LANES), 0) == iota((per, LANES), 1)

    for o in range(C):
        part = slice(o * per, (o + 1) * per)
        hot = lane_hot[part, :]
        for k in range(ITERS):
            mine = picked[pl.ds(o * per * ITERS + k, per, stride=ITERS), :]
            value = jnp.sum(mine * hot, axis=1, keepdims=True)
            seen_out[o + 1, k : k + 1, :] = jnp.sum(jnp.where(diag_hit, value, 0.0), axis=0, keepdims=True)
    seen_out[0] = seen_out[C]
    seen_out[C + 1] = seen_out[1]
    seen_row[col] = seen_out[pl.ds(col, 3)]
    seen_side = Batch(always, always, [
        (seen_out.at[pl.ds(lax.rem(col + d, C), 3)], seen_row.at[col], (row, lax.rem(col + d, C)))
        for d in range(1, C)
    ])
    seen_up = Batch(top_ok, bot_ok, [
        (seen_out.at[lax.rem(col + d, C) + 1], seen_ud.at[1, col], (up, lax.rem(col + d, C)))
        for d in range(C)
    ])
    seen_down = Batch(bot_ok, top_ok, [
        (seen_out.at[lax.rem(col + d, C) + 1], seen_ud.at[0, col], (down, lax.rem(col + d, C)))
        for d in range(C)
    ])

    for batch in pending[:early]:
        batch.leave()
    reductions.land()
    parts = [red_in[n] for n in range(R * C)]
    while len(parts) > 1:
        parts = [sum(parts[n : n + 2][1:], parts[n]) for n in range(0, len(parts), 2)]
    total = jnp.broadcast_to(parts[0], (8, LANES))
    total = jnp.sum(jnp.where(sub == lane_row, total, 0.0), axis=1, keepdims=True)
    scalar = [total[n : n + 1, :] for n in range(number)]
    energy = [scalar[1], scalar[2]] + scalar[3 : 3 + ITERS - 2]
    high = scalar[3 + ITERS - 2 :]
    for j in range(1, ITERS):
        energy.append(2.0 * high[j - 1] - energy[ITERS - 1 - j])
    moment = [scalar[0], scalar[0] - energy[0]]
    for n in range(2, ITERS):
        moment.append(2.0 * (moment[n - 1] - energy[n - 1]) - moment[n - 2])
    matrix = [[None] * (ITERS + 1) for _ in range(ITERS)]
    for j in range(ITERS):
        for k in range(j + 1):
            matrix[j][k] = matrix[k][j] = 0.5 * (energy[j + k] + energy[j - k])
        matrix[j][ITERS] = moment[j]
    for i in range(ITERS):
        inverse = 1.0 / matrix[i][i]
        for k in range(i + 1, ITERS + 1):
            matrix[i][k] = matrix[i][k] * inverse
        for j in range(i + 1, ITERS):
            for k in range(i + 1, ITERS + 1):
                matrix[j][k] = matrix[j][k] - matrix[j][i] * matrix[i][k]
    coef = [None] * ITERS
    for i in reversed(range(ITERS)):
        coef[i] = matrix[i][ITERS]
        for k in range(i + 1, ITERS):
            coef[i] = coef[i] - matrix[i][k] * coef[k]
    coef = [jnp.broadcast_to(c, (1, LANES)) for c in coef]

    def finish(i, carry):
        at = pl.ds(pl.multiple_of(i * step, step), step)
        for b in range(NB):
            inner = pl.ds(pl.multiple_of(b * EXT + PAD + i * step, 8), step)
            value = coef[0] * V[0, inner, :]
            for k in range(1, ITERS):
                value = value + coef[k] * V[k, inner, :]
            x_out[at, b * LANES : (b + 1) * LANES] = value
        return carry

    lax.fori_loop(0, TR // step, finish, 0)

    for n in range(2):
        coarse_land(coarse_later[n], n + 1)
    seen_side.land()
    seen_down.land(quiet(seen_ud.at[0], (ITERS, per)))
    seen_up.land(quiet(seen_ud.at[1], (ITERS, per)))

    def amount(value, weights):
        def one(t):
            seen = value(t)
            total = coef[0] * seen[0:1, :]
            for k in range(1, ITERS):
                total = total + coef[k] * seen[k : k + 1, :]
            return total * weights(t)
        return joined(one)

    def gathered(hit, value, weights, hot):
        out = dot_t(spread(hit, amount(value, weights)), hot)
        return out[: out.shape[0] // 2] + out[out.shape[0] // 2 :]

    place_g = iota((groups, S), 0) * GROUP
    one_row = iota((8, S), 0) == 0
    own_row, own_col = places(lambda t: msg_row[t, 1, 0:1, :])
    sources = gathered(
        place_r == own_row, lambda t: seen_row[t, 1], lambda t: msg_row[t, 1, 1:2, :], hot_own[...]
    )
    from_left = gathered(
        place_g + (GROUP - 1) == left_col, lambda t: seen_row[t, 0], lambda t: msg_row[t, 0, 1:2, :],
        hot_left[...],
    )
    from_right = gathered(
        place_g == right_col, lambda t: seen_row[t, 2], lambda t: msg_row[t, 2, 1:2, :], hot_right[...]
    )
    from_above = gathered(
        one_row & (above_row == BR - 1), lambda t: seen_ud[0, t], lambda t: msg_ud[0, t, 1:2, :], hot_up[...]
    )
    from_below = gathered(
        one_row & (below_row == 0), lambda t: seen_ud[1, t], lambda t: msg_ud[1, t, 1:2, :], hot_down[...]
    )
    scale = coarse[1]
    volt = coarse[0] + scale * sources
    sides = beside(
        volt, 0,
        crow_top[1, 7:8, :] + crow_top[2, 7:8, :] * from_above[0:1, :],
        crow_bot[1, 0:1, :] + crow_bot[2, 0:1, :] * from_below[0:1, :],
        cleft[1] + cleft[2] * from_left,
        cright[1] + cright[2] * from_right,
    )
    c_out[...] = volt + scale * (sources + coarse_conductance * sides - coarse[2] * volt)
    for batch in pending[early:]:
        batch.leave()


def per_device(R, C, load_amp, load_mask, leak, coarse_leak, coarse_init, via_fine, via_coarse, via_count):
    TR, TC = leak.shape
    BR, BC = coarse_leak.shape
    S = via_fine.shape[1]
    per = S // C
    NB = TC // LANES
    EXT = TR + 2 * PAD
    groups = BC // GROUP
    copies = 3 * (C - 1) + 4 * C + 2 * (2 + 2 * (2 + NB)) + 12 + R * C - 1
    vmem = pl.BlockSpec(memory_space=pltpu.VMEM)
    return pl.pallas_call(
        functools.partial(kernel, R, C),
        out_shape=(pltpu.VMEM((TR, TC), F32), pltpu.VMEM((BR, BC), F32)),
        in_specs=[pl.BlockSpec(memory_space=pltpu.HBM)] * 8,
        out_specs=(vmem, vmem),
        scratch_shapes=[
            pltpu.VMEM((NB, TR, LANES), F32), pltpu.VMEM((NB, TR, LANES), jnp.int32),
            pltpu.VMEM((NB, TR, LANES), F32),
            pltpu.VMEM((BR, BC), F32), pltpu.VMEM((BR, BC), F32),
            pltpu.VMEM((1, S), jnp.int32), pltpu.VMEM((1, S), jnp.int32),
            pltpu.SMEM((1, C), jnp.int32), pltpu.SemaphoreType.DMA((3 * NB + 6,)),
            pltpu.VMEM((C + 2, 2, per), F32), pltpu.VMEM((C, 3, 2, per), F32), pltpu.VMEM((2, C, 2, per), F32),
            pltpu.VMEM((C, 1, per), F32), pltpu.VMEM((C, 1, per), F32),
            pltpu.VMEM((C + 2, ITERS, per), F32), pltpu.VMEM((C, 3, ITERS, per), F32),
            pltpu.VMEM((2, C, ITERS, per), F32),
            pltpu.VMEM((1, S), jnp.int32), pltpu.SMEM((1, S), jnp.int32),
            pltpu.VMEM((NB * TR * ITERS, LANES), F32),
            pltpu.VMEM((ITERS * S, LANES), F32), pltpu.VMEM((S, LANES), F32),
            pltpu.VMEM((TR, S), BF16),
            pltpu.VMEM((S, TC), BF16),
            pltpu.VMEM((NB * EXT, LANES), F32),
            pltpu.VMEM((NB * TR, LANES), F32),
            pltpu.VMEM((EXT, LANES), F32),
            pltpu.VMEM((TR, LANES), F32),
            pltpu.VMEM((ITERS, NB * EXT, LANES), F32),
            pltpu.VMEM((ITERS, EXT, LANES), F32),
            pltpu.VMEM((NB * TR, LANES), F32),
            pltpu.VMEM((NB * TR, LANES), F32),
            pltpu.VMEM((TR, LANES), F32),
            pltpu.VMEM((2, TR, LANES), F32),
            pltpu.VMEM((2, LANES, TR), F32),
            pltpu.VMEM((2, LANES, TR), F32),
            pltpu.VMEM((2, NB, EDGE, LANES), F32),
            pltpu.VMEM((2, NB, EDGE, LANES), F32),
            pltpu.VMEM((2, 4, EDGE, LANES), F32),
            pltpu.VMEM((1, LANES), F32), pltpu.VMEM((R * C, 1, LANES), F32),
            pltpu.VMEM((BC, S), BF16), pltpu.VMEM((BR, S), BF16), pltpu.VMEM((BR, S), BF16),
            pltpu.VMEM((BC, S), BF16), pltpu.VMEM((BC, S), BF16),
            pltpu.VMEM((3, BR, BC), F32),
            pltpu.VMEM((3, BC, BR), F32), pltpu.VMEM((3, 2, groups, BR), F32),
            pltpu.VMEM((3, 8, BC), F32), pltpu.VMEM((3, 8, BC), F32),
            pltpu.VMEM((3, groups, BR), F32), pltpu.VMEM((3, groups, BR), F32),
            pltpu.SemaphoreType.DMA((copies,)),
            pltpu.SemaphoreType.DMA((copies,)),
        ],
        compiler_params=pltpu.CompilerParams(
            collective_id=0, has_side_effects=True, vmem_limit_bytes=58000 * 1024
        ),
    )(load_amp, load_mask, leak, coarse_leak, coarse_init, via_fine, via_coarse, via_count)


def solution(mesh):
    spec = P("row", "col")
    return jax.shard_map(
        functools.partial(per_device, mesh.shape["row"], mesh.shape["col"]),
        mesh=mesh, in_specs=(spec,) * 8, out_specs=(spec, spec), check_vma=False,
    )
```

```python
import functools
import jax
import jax.numpy as jnp
from jax import lax
from jax.experimental import pallas as pl
from jax.experimental.pallas import tpu as pltpu
from jax.sharding import PartitionSpec as P

GROUP = 16
ITERS = 4
LANES = 128
PAD = 16
EDGE = 8
HALF = LANES // 2
QUARTER = LANES // 4

via_conductance = 2.0
coarse_conductance = 4.0
relaxation = 0.8

F32 = jnp.float32
BF16 = jnp.bfloat16
MESH = pl.DeviceIdType.MESH


def divide(value, by):
    if by & (by - 1) == 0:
        return lax.shift_right_logical(value, by.bit_length() - 1)
    return value // by


def remainder(value, by):
    if by & (by - 1) == 0:
        return value & (by - 1)
    return value % by


def halves(value):
    high = value.astype(BF16).astype(F32)
    return high.astype(BF16), (value - high).astype(BF16)


def dot(a, b):
    return jnp.dot(a, b, preferred_element_type=F32)


def dot_t(a, b):
    return lax.dot_general(a, b, (((1,), (1,)), ((), ())), preferred_element_type=F32)


def fold(value):
    total = value[0:8]
    for n in range(1, value.shape[0] // 8):
        total = total + value[n * 8 : (n + 1) * 8]
    return total


def iota(shape, dim):
    return lax.broadcasted_iota(jnp.int32, shape, dim)


def kernel(
    R, C,
    amp_in, mask_in, leak_in, cleak_in, cinit_in, vf_in, vc_in, cnt_in,
    x_out, c_out,
    amp, mask, leak, cleak, cinit, vf, vc, cnt, load_sem,
    msg_out, msg_row, msg_ud, val_out, val_in, seen_out, seen_row, seen_ud,
    spot_v, spot, woven, picked, lane_hot,
    row_hot, Bt, dv, D, dvq, Dq, V, Q, R0, rhs, rhsq,
    E, ET, H, rtop, rbot, rcorner,
    red_out, red_in,
    hot_own, hot_left, hot_right, hot_up, hot_down,
    coarse, turn, seam_out, crow_top, crow_bot, cleft, cright,
    send_sem, recv_sem,
):
    row, col = lax.axis_index("row"), lax.axis_index("col")
    TR, TC = leak_in.shape
    NB = TC // LANES
    EXT = TR + 2 * PAD
    BR, BC = cleak.shape
    S = vf.shape[1]
    per = S // C
    groups = BC // GROUP

    def cut(b):
        return pl.ds(b * LANES, LANES)

    loads = []

    def load(source, target):
        copy = pltpu.make_async_copy(source, target, load_sem.at[len(loads)])
        copy.start()
        loads.append(copy)
        return copy

    def load_blocks(source, target):
        sem = load_sem.at[len(loads)]
        for b in range(NB):
            pltpu.make_async_copy(source.at[:, cut(b)], target.at[b], sem).start()
        copy = pltpu.make_async_copy(target, target, sem)
        loads.append(copy)
        return copy

    small = [load(cnt_in, cnt), load(vc_in, vc), load(vf_in, vf)]
    cinit_load = load(cinit_in, cinit.at[0])
    leak_load = load_blocks(leak_in, leak)
    cleak_load = load(cleak_in, cleak)
    amp_loads = [load_blocks(amp_in, amp), load_blocks(mask_in, mask)]

    up, down = lax.rem(row + R - 1, R), lax.rem(row + 1, R)
    left, right = lax.rem(col + C - 1, C), lax.rem(col + 1, C)
    top_ok, bot_ok = row > 0, row < R - 1
    left_ok, right_ok = col > 0, col < C - 1
    always = None

    barrier = pltpu.get_barrier_semaphore()

    def greet(r, c):
        pl.semaphore_signal(barrier, inc=1, device_id=(r, c), device_id_type=MESH)

    for d in range(1, C):
        greet(row, lax.rem(col + d, C))
    near_rows = R <= 4
    if near_rows:

        @pl.when(top_ok)
        def _():
            greet(up, col)

        @pl.when(bot_ok)
        def _():
            greet(down, col)
    else:
        for e in range(1, R):
            for d in range(C):
                greet(lax.rem(row + e, R), lax.rem(col + d, C))

    def welcome():
        if near_rows:
            rows = jnp.where(top_ok, 1, 0) + jnp.where(bot_ok, 1, 0)
            pl.semaphore_wait(barrier, C - 1 + rows)
        else:
            pl.semaphore_wait(barrier, R * C - 1)

    count = [0]
    pending = []

    def under(ok, body):
        if ok is always:
            body()
        else:
            pl.when(ok)(body)

    class Batch:
        def __init__(self, ok, heard, whole, specs):
            self.ok, self.heard = ok, heard
            n = count[0]
            count[0] += 1

            def make(src, dst, device):
                return pltpu.make_async_remote_copy(
                    src_ref=src, dst_ref=dst, send_sem=send_sem.at[n], recv_sem=recv_sem.at[n],
                    device_id=device, device_id_type=MESH,
                )

            self.all = make(whole, whole, specs[0][2])
            pending.append(self)

            def start():
                for spec in specs:
                    make(*spec).start()

            under(ok, start)

        def land(self, otherwise=None):
            under(self.heard, self.all.wait_recv)
            if self.heard is not always and otherwise is not None:
                pl.when(jnp.logical_not(self.heard))(otherwise)

        def leave(self):
            under(self.ok, self.all.wait_send)

    for copy in small:
        copy.wait()
    lane = iota((1, per), 1)
    weight = jnp.concatenate(
        [jnp.where(lane < cnt[0, o], via_conductance, 0.0).astype(F32) for o in range(C)], axis=1
    )
    node = vc[...].astype(F32)
    for o in [-1] + list(range(C)) + [C]:
        part = slice((o % C) * per, (o % C + 1) * per)
        msg_out[o + 1, 0:1, :] = node[:, part]
        msg_out[o + 1, 1:2, :] = weight[:, part]
    msg_row[col] = msg_out[pl.ds(col, 3)]
    fine = vf[...]
    fine_row = divide(fine, TC)
    fine_col = remainder(fine, TC)
    spot_v[...] = (divide(fine_col, LANES) * TR + fine_row) * ITERS
    spot_copy = pltpu.make_async_copy(spot_v, spot, load_sem.at[len(loads)])
    spot_copy.start()
    step = 64

    def build_rows(i, carry):
        at = pl.ds(pl.multiple_of(i * step, step), step)
        place = iota((step, S), 0) + i * step
        row_hot[at, :] = jnp.where(place == fine_row, 1.0, 0.0).astype(BF16)
        return carry

    lax.fori_loop(0, TR // step, build_rows, 0)

    welcome()

    messages = Batch(always, always, msg_row.at[pl.ds(0, C - 1)], [
        (msg_out.at[pl.ds(lax.rem(col + d, C), 3)], msg_row.at[col], (row, lax.rem(col + d, C)))
        for d in range(1, C)
    ])

    def seams(volt, n):
        turn[n] = volt.T
        seam_out[n, 0] = turn[n, pl.ds(0, groups, stride=GROUP), :]
        seam_out[n, 1] = turn[n, pl.ds(GROUP - 1, groups, stride=GROUP), :]

    def coarse_send(rows, n, m):
        at = pl.ds(n, m)
        return [
            Batch(top_ok, bot_ok, crow_bot.at[at], [(rows.at[:, pl.ds(0, 8)], crow_bot.at[at], (up, col))]),
            Batch(bot_ok, top_ok, crow_top.at[at], [(rows.at[:, pl.ds(BR - 8, 8)], crow_top.at[at], (down, col))]),
            Batch(always, always, seam_out.at[at], [
                (seam_out.at[at, 0], cright.at[at], (row, left)),
                (seam_out.at[at, 1], cleft.at[at], (row, right)),
            ]),
        ]

    def coarse_land(batches, n, m):
        def no_below():
            crow_bot[n : n + m] = jnp.zeros((m, 8, BC), F32)

        def no_above():
            crow_top[n : n + m] = jnp.zeros((m, 8, BC), F32)

        batches[0].land(no_below)
        batches[1].land(no_above)
        batches[2].land()

    cinit_load.wait()
    seams(cinit[0], 0)
    coarse0 = coarse_send(cinit, 0, 1)
    lanes = iota((per, LANES), 1).astype(F32)
    for o in range(C):
        part = slice(o * per, (o + 1) * per)
        turned = jnp.broadcast_to(fine_col[:, part].astype(F32), (LANES, per)).T
        near = turned
        total = jnp.zeros((per, LANES), F32)
        for b in range(NB):
            hot = jnp.where(turned == lanes + b * LANES, 1.0, 0.0)
            Bt[part, b * LANES : (b + 1) * LANES] = hot.astype(BF16)
            total = total + hot
        lane_hot[part, :] = total

    zero_pad = jnp.zeros((8, LANES), F32)
    for n in range(ITERS):
        for b in range(NB):
            V[n, b * EXT : b * EXT + 8, :] = zero_pad
            V[n, (b + 1) * EXT - 8 : (b + 1) * EXT, :] = zero_pad
        for b in range(NB if n == 0 else 0):
            V[n, b * EXT + 8 : b * EXT + 16, :] = zero_pad
            V[n, (b + 1) * EXT - 16 : (b + 1) * EXT - 8, :] = zero_pad
        Q[n, 0:8, :] = zero_pad
        Q[n, EXT - 8 : EXT, :] = zero_pad
    for n in range(1, ITERS):
        for b in range(NB):
            V[n, b * EXT + 8 : b * EXT + 16, :] = zero_pad
            V[n, (b + 1) * EXT - 16 : (b + 1) * EXT - 8, :] = zero_pad

    leak_load.wait()
    wide_step = 256 if TR % 256 == 0 else step
    weight_low = weight.astype(BF16)

    def diagonal(i, carry):
        at = pl.ds(pl.multiple_of(i * wide_step, wide_step), wide_step)
        sums = dot(row_hot[at, :] * weight_low, Bt[...])
        for b in range(NB):
            inner = pl.ds(pl.multiple_of(b * EXT + PAD + i * wide_step, 8), wide_step)
            own = pl.ds(pl.multiple_of(b * TR + i * wide_step, 8), wide_step)
            value = 4.0 + leak[b, at, :] + sums[:, b * LANES : (b + 1) * LANES]
            D[own, :] = value
            dv[inner, :] = 1.0 / value
        return carry

    lax.fori_loop(0, TR // wide_step, diagonal, 0)

    lane_row = iota((8, LANES), 1)

    def wide(rows):
        return iota((rows, LANES), 1)

    def keep(ok, value):
        return value * jnp.where(ok, 1.0, 0.0).astype(F32)

    last = (NB - 1) * EXT

    def halo_send(F, n):
        edge = jnp.where(wide(TR) < HALF, F[PAD : PAD + TR, :], F[last + PAD : last + PAD + TR, :])
        E[n] = edge
        ET[n] = edge.T
        sides = Batch(always, always, ET.at[n, pl.ds(0, 2 * EDGE)], [
            (ET.at[n, pl.ds(0, EDGE)], H.at[n, pl.ds(HALF, EDGE)], (row, left)),
            (ET.at[n, pl.ds(LANES - EDGE, EDGE)], H.at[n, pl.ds(LANES - EDGE, EDGE)], (row, right)),
        ])
        above = Batch(top_ok, bot_ok, rbot.at[n], [
            (F.at[pl.ds(b * EXT + PAD, EDGE)], rbot.at[n, b], (up, col)) for b in range(NB)
        ])
        below = Batch(bot_ok, top_ok, rtop.at[n], [
            (F.at[pl.ds(b * EXT + PAD + TR - EDGE, EDGE)], rtop.at[n, b], (down, col)) for b in range(NB)
        ])
        return sides, above, below

    def corner_send(n):
        above = Batch(top_ok, bot_ok, rcorner.at[n, pl.ds(2, 2)], [
            (E.at[n, pl.ds(0, EDGE)], rcorner.at[n, 3], (up, left)),
            (E.at[n, pl.ds(0, EDGE)], rcorner.at[n, 2], (up, right)),
        ])
        below = Batch(bot_ok, top_ok, rcorner.at[n, pl.ds(0, 2)], [
            (E.at[n, pl.ds(TR - EDGE, EDGE)], rcorner.at[n, 1], (down, left)),
            (E.at[n, pl.ds(TR - EDGE, EDGE)], rcorner.at[n, 0], (down, right)),
        ])
        return above, below

    def edges_of(first, final, beyond):
        rows = first.shape[0]
        place = wide(rows)
        own = jnp.where(place < QUARTER, first, pltpu.roll(final, HALF, 1))
        if beyond is None:
            return own
        return jnp.where(place < HALF, own, beyond)

    def outer(right_side, left_side):
        place = wide(right_side.shape[0])
        right_side = jnp.where((place < HALF + EDGE) & right_ok, right_side, 0.0)
        return jnp.where((place >= LANES - EDGE) & left_ok, left_side, right_side)

    def halo_land(F, X, n, batches):
        sides, above, below = batches
        sides.land()
        side = H[n].T
        X[PAD : PAD + TR, :] = edges_of(
            F[PAD : PAD + TR, :], F[last + PAD : last + PAD + TR, :], outer(side, side)
        )

        def no_below():
            for b in range(NB):
                F[b * EXT + PAD + TR : b * EXT + PAD + TR + EDGE, :] = zero_pad

        def no_above():
            for b in range(NB):
                F[b * EXT + PAD - EDGE : b * EXT + PAD, :] = zero_pad

        above.land(no_below)
        below.land(no_above)

        @pl.when(bot_ok)
        def _():
            for b in range(NB):
                F[b * EXT + PAD + TR : b * EXT + PAD + TR + EDGE, :] = rbot[n, b]

        @pl.when(top_ok)
        def _():
            for b in range(NB):
                F[b * EXT + PAD - EDGE : b * EXT + PAD, :] = rtop[n, b]

    def corner_land(X, n, batches):
        above, below = batches

        def no_below():
            X[PAD + TR : PAD + TR + EDGE, :] = zero_pad

        def no_above():
            X[PAD - EDGE : PAD, :] = zero_pad

        above.land(no_below)
        below.land(no_above)

        @pl.when(bot_ok)
        def _():
            beyond = outer(pltpu.roll(rcorner[n, 3], HALF, 1), rcorner[n, 2])
            X[PAD + TR : PAD + TR + EDGE, :] = edges_of(rbot[n, 0], rbot[n, NB - 1], beyond)

        @pl.when(top_ok)
        def _():
            beyond = outer(pltpu.roll(rcorner[n, 1], HALF, 1), rcorner[n, 0])
            X[PAD - EDGE : PAD, :] = edges_of(rtop[n, 0], rtop[n, NB - 1], beyond)

    dinv_copies = halo_send(dv, 0)

    messages.land()

    def joined(pick):
        return jnp.concatenate([pick(t) for t in range(C)], axis=1)

    def places(pick):
        code = joined(pick).astype(jnp.int32)
        return divide(code, BC * C), remainder(code, BC)

    place_r = iota((BR, S), 0)
    place_c = iota((BC, S), 0)

    def one_hot(hit):
        return jnp.where(hit, 1.0, 0.0).astype(BF16)

    in_row, in_col = places(lambda t: msg_row[t, 1, 0:1, :])
    in_weight = joined(lambda t: msg_row[t, 1, 1:2, :])
    row_hit = place_r == in_row
    col_hot = one_hot(place_c == in_col)
    hot_own[...] = col_hot
    hi, lo = halves(cinit[0])
    seen = dot(hi, col_hot) + dot(lo, col_hot)
    at_via = jnp.sum(jnp.where(row_hit, seen, 0.0), axis=0, keepdims=True)
    for t in range(C):
        val_out[t] = at_via[:, t * per : (t + 1) * per]
    val_in[col] = val_out[col]
    values = Batch(always, always, val_in.at[pl.ds(0, C - 1)], [
        (val_out.at[lax.rem(col + d, C)], val_in.at[col], (row, lax.rem(col + d, C)))
        for d in range(1, C)
    ])

    def spread(hit, amount):
        hi, lo = halves(amount)
        zero = jnp.zeros((), BF16)
        return jnp.concatenate([jnp.where(hit, hi, zero), jnp.where(hit, lo, zero)], axis=0)

    messages_up = Batch(top_ok, bot_ok, msg_ud.at[1], [
        (msg_out.at[lax.rem(col + d, C) + 1], msg_ud.at[1, col], (up, lax.rem(col + d, C)))
        for d in range(C)
    ])
    messages_down = Batch(bot_ok, top_ok, msg_ud.at[0], [
        (msg_out.at[lax.rem(col + d, C) + 1], msg_ud.at[0, col], (down, lax.rem(col + d, C)))
        for d in range(C)
    ])

    dinv_corners = corner_send(0)

    cleak_load.wait()
    only = jnp.where(row_hit, in_weight, 0.0).astype(BF16)
    coarse_diag = 4.0 * coarse_conductance + cleak[...] + dot_t(only, col_hot)
    scale = relaxation / coarse_diag
    place = iota((BR, BC), 1)
    place_v = iota((BR, BC), 0)
    within = remainder(place, GROUP)
    group = iota((groups, BR), 0)

    def beside(volt, n, above, below, far_left, far_right):
        above = jnp.where(place_v == 0, keep(top_ok, above), pltpu.roll(volt, 1, 0))
        below = jnp.where(place_v == BR - 1, keep(bot_ok, below), pltpu.roll(volt, BR - 1, 0))
        turn[n, pl.ds(0, groups, stride=GROUP), :] = jnp.where(
            left_ok, far_left, jnp.where(group == 0, 0.0, jnp.roll(far_left, 1, 0))
        )
        turn[n, pl.ds(GROUP - 1, groups, stride=GROUP), :] = jnp.where(
            right_ok, far_right, jnp.where(group == groups - 1, 0.0, jnp.roll(far_right, -1, 0))
        )
        edge = turn[n].T
        before = jnp.where(within == 0, edge, pltpu.roll(volt, 1, 1))
        after = jnp.where(within == GROUP - 1, edge, pltpu.roll(volt, BC - 1, 1))
        return above + below + before + after

    coarse_land(coarse0, 0, 1)
    volt = cinit[0]
    sides = beside(volt, 0, crow_top[0, 7:8, :], crow_bot[0, 0:1, :], cleft[0], cright[0])
    coarse[0] = volt + scale * (coarse_conductance * sides - coarse_diag * volt)
    coarse[1] = scale
    coarse[2] = coarse_diag
    for n in range(2):
        seams(coarse[n], n + 1)
    coarse_later = coarse_send(coarse.at[pl.ds(0, 2)], 1, 2)

    def quiet(ref, shape):
        def body():
            for t in range(C):
                ref[t] = jnp.zeros(shape, F32)
        return body

    left_row, left_col = places(lambda t: msg_row[t, 0, 0:1, :])
    right_row, right_col = places(lambda t: msg_row[t, 2, 0:1, :])
    hot_left[...] = one_hot(place_r == left_row)
    hot_right[...] = one_hot(place_r == right_row)

    def edge_copy(F, X, size):
        X[...] = edges_of(F[0:TR, :], F[(NB - 1) * size : (NB - 1) * size + TR, :], None)

    edge_copy(D, Dq, TR)
    halo_land(dv, dvq, 0, dinv_copies)

    for copy in amp_loads:
        copy.wait()
    values.land()
    drops = weight * joined(lambda o: val_in[o])
    drop_hi, drop_lo = halves(drops)
    half_step = TR

    def inject(i, carry):
        at = pl.ds(pl.multiple_of(i * half_step, half_step), half_step)
        hot = row_hot[at, :]
        added = dot(hot * drop_hi, Bt[...]) + dot(hot * drop_lo, Bt[...])
        for b in range(NB):
            inner = pl.ds(pl.multiple_of(b * EXT + PAD + i * half_step, 8), half_step)
            own = pl.ds(pl.multiple_of(b * TR + i * half_step, 8), half_step)
            value = amp[b, at, :] * mask[b, at, :].astype(F32) + added[:, b * LANES : (b + 1) * LANES]
            rhs[own, :] = value
            value = value * dv[inner, :]
            V[0, inner, :] = value
            woven[pl.ds((b * TR + i * half_step) * ITERS, half_step, stride=ITERS), :] = value
        return carry

    lax.fori_loop(0, TR // half_step, inject, 0)
    first_copies = halo_send(V.at[0], 1)
    corner_land(dvq, 0, dinv_corners)
    first_corners = corner_send(1)
    edge_copy(rhs, rhsq, TR)

    def stencil(k, start, size):
        place = wide(size)
        mids = [V[k, pl.ds(b * EXT + start, size), :] for b in range(NB)]
        lefts = [pltpu.roll(m, 1, 1) for m in mids]
        rights = [pltpu.roll(m, LANES - 1, 1) for m in mids]
        out = []
        for b in range(NB):
            tall = V[k, pl.ds(b * EXT + start - 1, size), :] + V[k, pl.ds(b * EXT + start + 1, size), :]
            before = jnp.where(place == 0, lefts[b - 1], lefts[b])
            after = jnp.where(place == LANES - 1, rights[(b + 1) % NB], rights[b])
            out.append(tall + (before + after))
        return mids, out

    def inward(b, value):
        place = wide(value.shape[0])
        if b == 0:
            value = jnp.where(place >= EDGE, value, 0.0)
        if b == NB - 1:
            value = jnp.where(place < LANES - EDGE, value, 0.0)
        return value

    def advance(k, start, size, totals, start0=None):
        start0 = start if start0 is None else start0
        mids, near = stencil(k, start, size)
        totals = None if totals is None else list(totals)
        for b in range(NB):
            at = pl.ds(b * EXT + start, size)
            own = pl.ds(b * TR + start - PAD, size)
            if k < ITERS - 1:
                fresh = dv[at, :] * near[b]
                if k:
                    fresh = (fresh + fresh) - V[k - 1, at, :]
                V[k + 1, at, :] = fresh
                if PAD <= start0 < PAD + TR:
                    woven[pl.ds((b * TR + start - PAD) * ITERS + k + 1, size, stride=ITERS), :] = fresh
                if totals is None:
                    continue
                if k == 0:
                    right_side = rhs[own, :]
                    applied = inward(b, right_side - near[b])
                    R0[own, :] = applied
                    totals[0] = totals[0] + fold(right_side * mids[b])
                    totals[1] = totals[1] + fold(applied * mids[b])
                    totals[2] = totals[2] + fold(applied * fresh)
                else:
                    totals[0] = totals[0] + fold(R0[own, :] * fresh)
            elif totals is not None:
                applied = inward(b, D[own, :] * mids[b] - near[b])
                totals[ITERS - 2] = totals[ITERS - 2] + fold(applied * mids[b])
                for j in range(1, ITERS - 1):
                    totals[j - 1] = totals[j - 1] + fold(applied * V[j, at, :])
        return None if totals is None else tuple(totals)

    def blank(n):
        return tuple(jnp.zeros((8, LANES), F32) for _ in range(n))

    kept = [3] + [1] * (ITERS - 2) + [ITERS - 1]
    inside = TR - 2 * EDGE
    chunk = inside // 2 if inside % 16 == 0 else inside
    sums = []
    for k in range(ITERS):
        if k < ITERS - 1:
            advance(k, PAD, EDGE, None)
            advance(k, PAD + TR - EDGE, EDGE, None)

        def body(i, carry, k=k):
            return advance(k, PAD + EDGE + i * chunk, chunk, carry, PAD)

        sums.append(lax.fori_loop(0, inside // chunk, body, blank(kept[k])))

    halo_land(V.at[0], Q.at[0], 1, first_copies)
    corner_land(Q.at[0], 1, first_corners)
    def rim(value):
        place = wide(value.shape[0])
        ours = (place < EDGE) | ((place >= HALF - EDGE) & (place < HALF))
        return jnp.where(ours, value, 0.0)

    def advance_edge(k, start, size, totals):
        mid = Q[k, pl.ds(start, size), :]
        near = Q[k, pl.ds(start - 1, size), :] + Q[k, pl.ds(start + 1, size), :]
        near = near + (pltpu.roll(mid, 1, 1) + pltpu.roll(mid, LANES - 1, 1))
        at = pl.ds(start, size)
        own = pl.ds(start - PAD, size)
        totals = None if totals is None else list(totals)
        if k < ITERS - 1:
            fresh = dvq[at, :] * near
            if k:
                fresh = (fresh + fresh) - Q[k - 1, at, :]
            Q[k + 1, at, :] = fresh
            if totals is not None:
                place = wide(size)
                value = jnp.where(place < EDGE, fresh, V[k + 1, at, :])
                V[k + 1, at, :] = value
                woven[pl.ds((start - PAD) * ITERS + k + 1, size, stride=ITERS), :] = value
                far = pl.ds(last + start, size)
                value = jnp.where(place >= LANES - EDGE, pltpu.roll(fresh, HALF, 1), V[k + 1, far, :])
                V[k + 1, far, :] = value
                woven[pl.ds(((NB - 1) * TR + start - PAD) * ITERS + k + 1, size, stride=ITERS), :] = value
                if k == 0:
                    applied = rim(rhsq[own, :] - near)
                    rhsq[own, :] = applied
                    totals[1] = totals[1] + fold(applied * mid)
                    totals[2] = totals[2] + fold(applied * fresh)
                else:
                    totals[0] = totals[0] + fold(rhsq[own, :] * fresh)
        elif totals is not None:
            applied = rim(Dq[own, :] * mid - near)
            totals[ITERS - 2] = totals[ITERS - 2] + fold(applied * mid)
            for j in range(1, ITERS - 1):
                totals[j - 1] = totals[j - 1] + fold(applied * Q[j, at, :])
        return None if totals is None else tuple(totals)

    for k in range(ITERS):
        if k < ITERS - 1:
            advance(k, PAD - EDGE, EDGE, None)
            advance(k, PAD + TR, EDGE, None)
            advance_edge(k, PAD - EDGE, EDGE, None)
            advance_edge(k, PAD + TR, EDGE, None)
        sums[k] = advance(k, PAD, EDGE, sums[k])
        sums[k] = advance(k, PAD + TR - EDGE, EDGE, sums[k])
        sums[k] = advance_edge(k, PAD, TR, sums[k])

    flat = [total for part in sums for total in part]
    tile = jnp.concatenate([jnp.sum(total, axis=0, keepdims=True) for total in flat], axis=0)
    sub = iota((8, LANES), 0)
    number = len(flat)
    tile = jnp.sum(tile, axis=1, keepdims=True)
    red_out[...] = jnp.sum(jnp.where(sub == lane_row, tile, 0.0), axis=0, keepdims=True)
    me = row * C + col
    early = len(pending)
    red_in[me] = red_out[...]
    reductions = Batch(always, always, red_in.at[pl.ds(0, R * C - 1)], [
        (red_out, red_in.at[me], (lax.rem(row + e, R), lax.rem(col + d, C)))
        for e in reversed(range(R)) for d in reversed(range(C)) if e or d
    ])

    spot_copy.wait()
    unroll = 32

    def pick(i, carry):
        for n in range(unroll):
            s = i * unroll + n
            where = spot[0, s]
            picked[pl.ds(pl.multiple_of(s * ITERS, ITERS), ITERS), :] = woven[pl.ds(where, ITERS), :]
        return carry

    lax.fori_loop(0, S // unroll, pick, 0)
    diag_hit = iota((per, LANES), 0) == iota((per, LANES), 1)

    for o in range(C):
        part = slice(o * per, (o + 1) * per)
        hot = lane_hot[part, :]
        for k in range(ITERS):
            mine = picked[pl.ds(o * per * ITERS + k, per, stride=ITERS), :]
            value = jnp.sum(mine * hot, axis=1, keepdims=True)
            seen_out[o + 1, k : k + 1, :] = jnp.sum(jnp.where(diag_hit, value, 0.0), axis=0, keepdims=True)
    seen_out[0] = seen_out[C]
    seen_out[C + 1] = seen_out[1]
    seen_row[col] = seen_out[pl.ds(col, 3)]
    seen_side = Batch(always, always, seen_row.at[pl.ds(0, C - 1)], [
        (seen_out.at[pl.ds(lax.rem(col + d, C), 3)], seen_row.at[col], (row, lax.rem(col + d, C)))
        for d in range(1, C)
    ])
    seen_up = Batch(top_ok, bot_ok, seen_ud.at[1], [
        (seen_out.at[lax.rem(col + d, C) + 1], seen_ud.at[1, col], (up, lax.rem(col + d, C)))
        for d in range(C)
    ])
    seen_down = Batch(bot_ok, top_ok, seen_ud.at[0], [
        (seen_out.at[lax.rem(col + d, C) + 1], seen_ud.at[0, col], (down, lax.rem(col + d, C)))
        for d in range(C)
    ])

    messages_down.land(quiet(msg_ud.at[0], (2, per)))
    messages_up.land(quiet(msg_ud.at[1], (2, per)))
    above_row, above_col = places(lambda t: msg_ud[0, t, 0:1, :])
    below_row, below_col = places(lambda t: msg_ud[1, t, 0:1, :])
    hot_up[...] = one_hot(place_c == above_col)
    hot_down[...] = one_hot(place_c == below_col)


    for batch in pending[:early]:
        batch.leave()
    reductions.land()
    parts = [red_in[n] for n in range(R * C)]
    while len(parts) > 1:
        parts = [sum(parts[n : n + 2][1:], parts[n]) for n in range(0, len(parts), 2)]
    total = jnp.broadcast_to(parts[0], (8, LANES))
    total = jnp.sum(jnp.where(sub == lane_row, total, 0.0), axis=1, keepdims=True)
    scalar = [total[n : n + 1, :] for n in range(number)]
    energy = [scalar[1], scalar[2]] + scalar[3 : 3 + ITERS - 2]
    high = scalar[3 + ITERS - 2 :]
    for j in range(1, ITERS):
        energy.append(2.0 * high[j - 1] - energy[ITERS - 1 - j])
    moment = [scalar[0], scalar[0] - energy[0]]
    for n in range(2, ITERS):
        moment.append(2.0 * (moment[n - 1] - energy[n - 1]) - moment[n - 2])
    matrix = [[None] * (ITERS + 1) for _ in range(ITERS)]
    for j in range(ITERS):
        for k in range(j + 1):
            matrix[j][k] = matrix[k][j] = 0.5 * (energy[j + k] + energy[j - k])
        matrix[j][ITERS] = moment[j]
    for i in range(ITERS):
        inverse = 1.0 / matrix[i][i]
        for k in range(i + 1, ITERS + 1):
            matrix[i][k] = matrix[i][k] * inverse
        for j in range(i + 1, ITERS):
            for k in range(i + 1, ITERS + 1):
                matrix[j][k] = matrix[j][k] - matrix[j][i] * matrix[i][k]
    coef = [None] * ITERS
    for i in reversed(range(ITERS)):
        coef[i] = matrix[i][ITERS]
        for k in range(i + 1, ITERS):
            coef[i] = coef[i] - matrix[i][k] * coef[k]
    coef = [jnp.broadcast_to(c, (1, LANES)) for c in coef]

    def finish(i, carry):
        at = pl.ds(pl.multiple_of(i * step, step), step)
        for b in range(NB):
            inner = pl.ds(pl.multiple_of(b * EXT + PAD + i * step, 8), step)
            value = coef[0] * V[0, inner, :]
            for k in range(1, ITERS):
                value = value + coef[k] * V[k, inner, :]
            x_out[at, b * LANES : (b + 1) * LANES] = value
        return carry

    lax.fori_loop(0, TR // step, finish, 0)

    coarse_land(coarse_later, 1, 2)
    seen_side.land()
    seen_down.land(quiet(seen_ud.at[0], (ITERS, per)))
    seen_up.land(quiet(seen_ud.at[1], (ITERS, per)))

    def amount(value, weights):
        def one(t):
            seen = value(t)
            total = coef[0] * seen[0:1, :]
            for k in range(1, ITERS):
                total = total + coef[k] * seen[k : k + 1, :]
            return total * weights(t)
        return joined(one)

    def gathered(hit, value, weights, hot):
        out = dot_t(spread(hit, amount(value, weights)), hot)
        return out[: out.shape[0] // 2] + out[out.shape[0] // 2 :]

    place_g = iota((groups, S), 0) * GROUP
    one_row = iota((8, S), 0) == 0
    own_row, own_col = places(lambda t: msg_row[t, 1, 0:1, :])
    sources = gathered(
        place_r == own_row, lambda t: seen_row[t, 1], lambda t: msg_row[t, 1, 1:2, :], hot_own[...]
    )
    from_left = gathered(
        place_g + (GROUP - 1) == left_col, lambda t: seen_row[t, 0], lambda t: msg_row[t, 0, 1:2, :],
        hot_left[...],
    )
    from_right = gathered(
        place_g == right_col, lambda t: seen_row[t, 2], lambda t: msg_row[t, 2, 1:2, :], hot_right[...]
    )
    from_above = gathered(
        one_row & (above_row == BR - 1), lambda t: seen_ud[0, t], lambda t: msg_ud[0, t, 1:2, :], hot_up[...]
    )
    from_below = gathered(
        one_row & (below_row == 0), lambda t: seen_ud[1, t], lambda t: msg_ud[1, t, 1:2, :], hot_down[...]
    )
    scale = coarse[1]
    volt = coarse[0] + scale * sources
    sides = beside(
        volt, 0,
        crow_top[1, 7:8, :] + crow_top[2, 7:8, :] * from_above[0:1, :],
        crow_bot[1, 0:1, :] + crow_bot[2, 0:1, :] * from_below[0:1, :],
        cleft[1] + cleft[2] * from_left,
        cright[1] + cright[2] * from_right,
    )
    c_out[...] = volt + scale * (sources + coarse_conductance * sides - coarse[2] * volt)
    assert count[0] == send_sem.shape[0]
    for batch in pending[early:]:
        batch.leave()


def per_device(R, C, load_amp, load_mask, leak, coarse_leak, coarse_init, via_fine, via_coarse, via_count):
    TR, TC = leak.shape
    BR, BC = coarse_leak.shape
    S = via_fine.shape[1]
    per = S // C
    NB = TC // LANES
    EXT = TR + 2 * PAD
    groups = BC // GROUP
    batches = 24
    vmem = pl.BlockSpec(memory_space=pltpu.VMEM)
    return pl.pallas_call(
        functools.partial(kernel, R, C),
        out_shape=(pltpu.VMEM((TR, TC), F32), pltpu.VMEM((BR, BC), F32)),
        in_specs=[pl.BlockSpec(memory_space=pltpu.HBM)] * 8,
        out_specs=(vmem, vmem),
        scratch_shapes=[
            pltpu.VMEM((NB, TR, LANES), F32), pltpu.VMEM((NB, TR, LANES), jnp.int32),
            pltpu.VMEM((NB, TR, LANES), F32),
            pltpu.VMEM((BR, BC), F32), pltpu.VMEM((1, BR, BC), F32),
            pltpu.VMEM((1, S), jnp.int32), pltpu.VMEM((1, S), jnp.int32),
            pltpu.SMEM((1, C), jnp.int32), pltpu.SemaphoreType.DMA((9,)),
            pltpu.VMEM((C + 2, 2, per), F32), pltpu.VMEM((C, 3, 2, per), F32), pltpu.VMEM((2, C, 2, per), F32),
            pltpu.VMEM((C, 1, per), F32), pltpu.VMEM((C, 1, per), F32),
            pltpu.VMEM((C + 2, ITERS, per), F32), pltpu.VMEM((C, 3, ITERS, per), F32),
            pltpu.VMEM((2, C, ITERS, per), F32),
            pltpu.VMEM((1, S), jnp.int32), pltpu.SMEM((1, S), jnp.int32),
            pltpu.VMEM((NB * TR * ITERS, LANES), F32),
            pltpu.VMEM((ITERS * S, LANES), F32), pltpu.VMEM((S, LANES), F32),
            pltpu.VMEM((TR, S), BF16),
            pltpu.VMEM((S, TC), BF16),
            pltpu.VMEM((NB * EXT, LANES), F32),
            pltpu.VMEM((NB * TR, LANES), F32),
            pltpu.VMEM((EXT, LANES), F32),
            pltpu.VMEM((TR, LANES), F32),
            pltpu.VMEM((ITERS, NB * EXT, LANES), F32),
            pltpu.VMEM((ITERS, EXT, LANES), F32),
            pltpu.VMEM((NB * TR, LANES), F32),
            pltpu.VMEM((NB * TR, LANES), F32),
            pltpu.VMEM((TR, LANES), F32),
            pltpu.VMEM((2, TR, LANES), F32),
            pltpu.VMEM((2, LANES, TR), F32),
            pltpu.VMEM((2, LANES, TR), F32),
            pltpu.VMEM((2, NB, EDGE, LANES), F32),
            pltpu.VMEM((2, NB, EDGE, LANES), F32),
            pltpu.VMEM((2, 4, EDGE, LANES), F32),
            pltpu.VMEM((1, LANES), F32), pltpu.VMEM((R * C, 1, LANES), F32),
            pltpu.VMEM((BC, S), BF16), pltpu.VMEM((BR, S), BF16), pltpu.VMEM((BR, S), BF16),
            pltpu.VMEM((BC, S), BF16), pltpu.VMEM((BC, S), BF16),
            pltpu.VMEM((3, BR, BC), F32),
            pltpu.VMEM((3, BC, BR), F32), pltpu.VMEM((3, 2, groups, BR), F32),
            pltpu.VMEM((3, 8, BC), F32), pltpu.VMEM((3, 8, BC), F32),
            pltpu.VMEM((3, groups, BR), F32), pltpu.VMEM((3, groups, BR), F32),
            pltpu.SemaphoreType.DMA((batches,)),
            pltpu.SemaphoreType.DMA((batches,)),
        ],
        compiler_params=pltpu.CompilerParams(
            collective_id=0, has_side_effects=True, vmem_limit_bytes=58000 * 1024
        ),
    )(load_amp, load_mask, leak, coarse_leak, coarse_init, via_fine, via_coarse, via_count)


def solution(mesh):
    spec = P("row", "col")
    return jax.shard_map(
        functools.partial(per_device, mesh.shape["row"], mesh.shape["col"]),
        mesh=mesh, in_specs=(spec,) * 8, out_specs=(spec, spec), check_vma=False,
    )
```

```python
import functools
import jax
import jax.numpy as jnp
from jax import lax
from jax.experimental import pallas as pl
from jax.experimental.pallas import tpu as pltpu
from jax.sharding import PartitionSpec as P

GROUP = 16
ITERS = 4
LANES = 128
PAD = 16
EDGE = 8
HALF = LANES // 2
QUARTER = LANES // 4

via_conductance = 2.0
coarse_conductance = 4.0
relaxation = 0.8

F32 = jnp.float32
BF16 = jnp.bfloat16
MESH = pl.DeviceIdType.MESH


def divide(value, by):
    if by & (by - 1) == 0:
        return lax.shift_right_logical(value, by.bit_length() - 1)
    return value // by


def remainder(value, by):
    if by & (by - 1) == 0:
        return value & (by - 1)
    return value % by


def halves(value):
    high = value.astype(BF16).astype(F32)
    return high.astype(BF16), (value - high).astype(BF16)


def dot(a, b):
    return jnp.dot(a, b, preferred_element_type=F32)


def dot_t(a, b):
    return lax.dot_general(a, b, (((1,), (1,)), ((), ())), preferred_element_type=F32)


def fold(value):
    total = value[0:8]
    for n in range(1, value.shape[0] // 8):
        total = total + value[n * 8 : (n + 1) * 8]
    return total


def iota(shape, dim):
    return lax.broadcasted_iota(jnp.int32, shape, dim)


def spread(hit, amount):
    hi, lo = halves(amount)
    zero = jnp.zeros((), BF16)
    return jnp.concatenate([jnp.where(hit, hi, zero), jnp.where(hit, lo, zero)], axis=0)


def beside(turn, R, C, volt, above, below, far_left, far_right):
    row, col = lax.axis_index("row"), lax.axis_index("col")
    BR, BC = volt.shape
    groups = BC // GROUP
    place_v = iota((BR, BC), 0)
    within = remainder(iota((BR, BC), 1), GROUP)
    group = iota((groups, BR), 0)
    above = jnp.where(place_v == 0, jnp.where(row > 0, above, 0.0), pltpu.roll(volt, 1, 0))
    below = jnp.where(place_v == BR - 1, jnp.where(row < R - 1, below, 0.0), pltpu.roll(volt, BR - 1, 0))
    turn[pl.ds(0, groups, stride=GROUP), :] = jnp.where(
        col > 0, far_left, jnp.where(group == 0, 0.0, jnp.roll(far_left, 1, 0))
    )
    turn[pl.ds(GROUP - 1, groups, stride=GROUP), :] = jnp.where(
        col < C - 1, far_right, jnp.where(group == groups - 1, 0.0, jnp.roll(far_right, -1, 0))
    )
    edge = turn[...].T
    before = jnp.where(within == 0, edge, pltpu.roll(volt, 1, 1))
    after = jnp.where(within == GROUP - 1, edge, pltpu.roll(volt, BC - 1, 1))
    return above + below + before + after


def kernel(
    R, C,
    amp_in, mask_in, leak_in, cleak_in, cinit_in, vf_in, vc_in, cnt_in,
    x_out, coef_out, nodes, basis, coarse, beyond_rows, beyond_cols,
    hot_own, hot_left, hot_right, hot_up, hot_down,
    amp, mask, leak, cleak, cinit, vf, vc, cnt, load_sem,
    msg_out, msg_row, msg_ud, val_out, val_in, seen_out, seen_row, seen_ud,
    spot_v, spot, woven, picked, lane_hot,
    row_hot, Bt, dv, D, dvq, Dq, V, Q, R0, rhs, rhsq,
    E, ET, H, rtop, rbot, rcorner,
    red_out, red_in,
    turn, seam_out, crow_top, crow_bot, cleft, cright,
    send_sem, recv_sem,
):
    row, col = lax.axis_index("row"), lax.axis_index("col")
    TR, TC = leak_in.shape
    NB = TC // LANES
    EXT = TR + 2 * PAD
    BR, BC = cleak.shape
    S = vf.shape[1]
    per = S // C
    groups = BC // GROUP

    def cut(b):
        return pl.ds(b * LANES, LANES)

    loads = []

    def load(source, target):
        copy = pltpu.make_async_copy(source, target, load_sem.at[len(loads)])
        copy.start()
        loads.append(copy)
        return copy

    def load_blocks(source, target):
        sem = load_sem.at[len(loads)]
        for b in range(NB):
            pltpu.make_async_copy(source.at[:, cut(b)], target.at[b], sem).start()
        copy = pltpu.make_async_copy(target, target, sem)
        loads.append(copy)
        return copy

    small = [load(cnt_in, cnt), load(vc_in, vc), load(vf_in, vf)]
    cinit_load = load(cinit_in, cinit.at[0])
    leak_load = load_blocks(leak_in, leak)
    cleak_load = load(cleak_in, cleak)
    amp_loads = [load_blocks(amp_in, amp), load_blocks(mask_in, mask)]

    up, down = lax.rem(row + R - 1, R), lax.rem(row + 1, R)
    left, right = lax.rem(col + C - 1, C), lax.rem(col + 1, C)
    top_ok, bot_ok = row > 0, row < R - 1
    left_ok, right_ok = col > 0, col < C - 1
    always = None

    barrier = pltpu.get_barrier_semaphore()

    def greet(r, c):
        pl.semaphore_signal(barrier, inc=1, device_id=(r, c), device_id_type=MESH)

    for d in range(1, C):
        greet(row, lax.rem(col + d, C))
    near_rows = R <= 4
    if near_rows:

        @pl.when(top_ok)
        def _():
            greet(up, col)

        @pl.when(bot_ok)
        def _():
            greet(down, col)
    else:
        for e in range(1, R):
            for d in range(C):
                greet(lax.rem(row + e, R), lax.rem(col + d, C))

    def welcome():
        if near_rows:
            rows = jnp.where(top_ok, 1, 0) + jnp.where(bot_ok, 1, 0)
            pl.semaphore_wait(barrier, C - 1 + rows)
        else:
            pl.semaphore_wait(barrier, R * C - 1)

    count = [0]
    pending = []

    def under(ok, body):
        if ok is always:
            body()
        else:
            pl.when(ok)(body)

    class Batch:
        def __init__(self, ok, heard, whole, specs):
            self.ok, self.heard = ok, heard
            n = count[0]
            count[0] += 1

            def make(src, dst, device):
                return pltpu.make_async_remote_copy(
                    src_ref=src, dst_ref=dst, send_sem=send_sem.at[n], recv_sem=recv_sem.at[n],
                    device_id=device, device_id_type=MESH,
                )

            self.all = make(whole, whole, specs[0][2])
            pending.append(self)

            def start():
                for spec in specs:
                    make(*spec).start()

            under(ok, start)

        def land(self, otherwise=None):
            under(self.heard, self.all.wait_recv)
            if self.heard is not always and otherwise is not None:
                pl.when(jnp.logical_not(self.heard))(otherwise)

        def leave(self):
            under(self.ok, self.all.wait_send)

    for copy in small:
        copy.wait()
    lane = iota((1, per), 1)
    weight = jnp.concatenate(
        [jnp.where(lane < cnt[0, o], via_conductance, 0.0).astype(F32) for o in range(C)], axis=1
    )
    node = vc[...].astype(F32)
    for o in [-1] + list(range(C)) + [C]:
        part = slice((o % C) * per, (o % C + 1) * per)
        msg_out[o + 1, 0:1, :] = node[:, part]
        msg_out[o + 1, 1:2, :] = weight[:, part]
    msg_row[col] = msg_out[pl.ds(col, 3)]
    fine = vf[...]
    fine_row = divide(fine, TC)
    fine_col = remainder(fine, TC)
    spot_v[...] = (divide(fine_col, LANES) * TR + fine_row) * ITERS
    spot_copy = pltpu.make_async_copy(spot_v, spot, load_sem.at[len(loads)])
    spot_copy.start()
    step = 64

    def build_rows(i, carry):
        at = pl.ds(pl.multiple_of(i * step, step), step)
        place = iota((step, S), 0) + i * step
        row_hot[at, :] = jnp.where(place == fine_row, 1.0, 0.0).astype(BF16)
        return carry

    lax.fori_loop(0, TR // step, build_rows, 0)

    welcome()

    messages = Batch(always, always, msg_row.at[pl.ds(0, C - 1)], [
        (msg_out.at[pl.ds(lax.rem(col + d, C), 3)], msg_row.at[col], (row, lax.rem(col + d, C)))
        for d in range(1, C)
    ])

    def seams(volt, n):
        turn[n] = volt.T
        seam_out[n, 0] = turn[n, pl.ds(0, groups, stride=GROUP), :]
        seam_out[n, 1] = turn[n, pl.ds(GROUP - 1, groups, stride=GROUP), :]

    def coarse_send(rows, n, m):
        at = pl.ds(n, m)
        return [
            Batch(top_ok, bot_ok, crow_bot.at[at], [(rows.at[:, pl.ds(0, 8)], crow_bot.at[at], (up, col))]),
            Batch(bot_ok, top_ok, crow_top.at[at], [(rows.at[:, pl.ds(BR - 8, 8)], crow_top.at[at], (down, col))]),
            Batch(always, always, seam_out.at[at], [
                (seam_out.at[at, 0], cright.at[at], (row, left)),
                (seam_out.at[at, 1], cleft.at[at], (row, right)),
            ]),
        ]

    def coarse_land(batches, n, m):
        def no_below():
            crow_bot[n : n + m] = jnp.zeros((m, 8, BC), F32)

        def no_above():
            crow_top[n : n + m] = jnp.zeros((m, 8, BC), F32)

        batches[0].land(no_below)
        batches[1].land(no_above)
        batches[2].land()

    cinit_load.wait()
    seams(cinit[0], 0)
    coarse0 = coarse_send(cinit, 0, 1)
    lanes = iota((per, LANES), 1).astype(F32)
    for o in range(C):
        part = slice(o * per, (o + 1) * per)
        turned = jnp.broadcast_to(fine_col[:, part].astype(F32), (LANES, per)).T
        near = turned
        total = jnp.zeros((per, LANES), F32)
        for b in range(NB):
            hot = jnp.where(turned == lanes + b * LANES, 1.0, 0.0)
            Bt[part, b * LANES : (b + 1) * LANES] = hot.astype(BF16)
            total = total + hot
        lane_hot[part, :] = total

    zero_pad = jnp.zeros((8, LANES), F32)
    for n in range(ITERS):
        for b in range(NB):
            V[n, b * EXT : b * EXT + 8, :] = zero_pad
            V[n, (b + 1) * EXT - 8 : (b + 1) * EXT, :] = zero_pad
        for b in range(NB if n == 0 else 0):
            V[n, b * EXT + 8 : b * EXT + 16, :] = zero_pad
            V[n, (b + 1) * EXT - 16 : (b + 1) * EXT - 8, :] = zero_pad
        Q[n, 0:8, :] = zero_pad
        Q[n, EXT - 8 : EXT, :] = zero_pad
    for n in range(1, ITERS):
        for b in range(NB):
            V[n, b * EXT + 8 : b * EXT + 16, :] = zero_pad
            V[n, (b + 1) * EXT - 16 : (b + 1) * EXT - 8, :] = zero_pad

    leak_load.wait()
    wide_step = 256 if TR % 256 == 0 else step
    weight_low = weight.astype(BF16)

    def diagonal(i, carry):
        at = pl.ds(pl.multiple_of(i * wide_step, wide_step), wide_step)
        sums = dot(row_hot[at, :] * weight_low, Bt[...])
        for b in range(NB):
            inner = pl.ds(pl.multiple_of(b * EXT + PAD + i * wide_step, 8), wide_step)
            own = pl.ds(pl.multiple_of(b * TR + i * wide_step, 8), wide_step)
            value = 4.0 + leak[b, at, :] + sums[:, b * LANES : (b + 1) * LANES]
            D[own, :] = value
            dv[inner, :] = 1.0 / value
        return carry

    lax.fori_loop(0, TR // wide_step, diagonal, 0)

    lane_row = iota((8, LANES), 1)

    def wide(rows):
        return iota((rows, LANES), 1)

    def keep(ok, value):
        return value * jnp.where(ok, 1.0, 0.0).astype(F32)

    last = (NB - 1) * EXT

    def halo_send(F, n):
        edge = jnp.where(wide(TR) < HALF, F[PAD : PAD + TR, :], F[last + PAD : last + PAD + TR, :])
        E[n] = edge
        ET[n] = edge.T
        sides = Batch(always, always, ET.at[n, pl.ds(0, 2 * EDGE)], [
            (ET.at[n, pl.ds(0, EDGE)], H.at[n, pl.ds(HALF, EDGE)], (row, left)),
            (ET.at[n, pl.ds(LANES - EDGE, EDGE)], H.at[n, pl.ds(LANES - EDGE, EDGE)], (row, right)),
        ])
        above = Batch(top_ok, bot_ok, rbot.at[n], [
            (F.at[pl.ds(b * EXT + PAD, EDGE)], rbot.at[n, b], (up, col)) for b in range(NB)
        ])
        below = Batch(bot_ok, top_ok, rtop.at[n], [
            (F.at[pl.ds(b * EXT + PAD + TR - EDGE, EDGE)], rtop.at[n, b], (down, col)) for b in range(NB)
        ])
        return sides, above, below

    def corner_send(n):
        above = Batch(top_ok, bot_ok, rcorner.at[n, pl.ds(2, 2)], [
            (E.at[n, pl.ds(0, EDGE)], rcorner.at[n, 3], (up, left)),
            (E.at[n, pl.ds(0, EDGE)], rcorner.at[n, 2], (up, right)),
        ])
        below = Batch(bot_ok, top_ok, rcorner.at[n, pl.ds(0, 2)], [
            (E.at[n, pl.ds(TR - EDGE, EDGE)], rcorner.at[n, 1], (down, left)),
            (E.at[n, pl.ds(TR - EDGE, EDGE)], rcorner.at[n, 0], (down, right)),
        ])
        return above, below

    def edges_of(first, final, beyond):
        rows = first.shape[0]
        place = wide(rows)
        own = jnp.where(place < QUARTER, first, pltpu.roll(final, HALF, 1))
        if beyond is None:
            return own
        return jnp.where(place < HALF, own, beyond)

    def outer(right_side, left_side):
        place = wide(right_side.shape[0])
        right_side = jnp.where((place < HALF + EDGE) & right_ok, right_side, 0.0)
        return jnp.where((place >= LANES - EDGE) & left_ok, left_side, right_side)

    def halo_land(F, X, n, batches):
        sides, above, below = batches
        sides.land()
        side = H[n].T
        X[PAD : PAD + TR, :] = edges_of(
            F[PAD : PAD + TR, :], F[last + PAD : last + PAD + TR, :], outer(side, side)
        )

        def no_below():
            for b in range(NB):
                F[b * EXT + PAD + TR : b * EXT + PAD + TR + EDGE, :] = zero_pad

        def no_above():
            for b in range(NB):
                F[b * EXT + PAD - EDGE : b * EXT + PAD, :] = zero_pad

        above.land(no_below)
        below.land(no_above)

        @pl.when(bot_ok)
        def _():
            for b in range(NB):
                F[b * EXT + PAD + TR : b * EXT + PAD + TR + EDGE, :] = rbot[n, b]

        @pl.when(top_ok)
        def _():
            for b in range(NB):
                F[b * EXT + PAD - EDGE : b * EXT + PAD, :] = rtop[n, b]

    def corner_land(X, n, batches):
        above, below = batches

        def no_below():
            X[PAD + TR : PAD + TR + EDGE, :] = zero_pad

        def no_above():
            X[PAD - EDGE : PAD, :] = zero_pad

        above.land(no_below)
        below.land(no_above)

        @pl.when(bot_ok)
        def _():
            beyond = outer(pltpu.roll(rcorner[n, 3], HALF, 1), rcorner[n, 2])
            X[PAD + TR : PAD + TR + EDGE, :] = edges_of(rbot[n, 0], rbot[n, NB - 1], beyond)

        @pl.when(top_ok)
        def _():
            beyond = outer(pltpu.roll(rcorner[n, 1], HALF, 1), rcorner[n, 0])
            X[PAD - EDGE : PAD, :] = edges_of(rtop[n, 0], rtop[n, NB - 1], beyond)

    dinv_copies = halo_send(dv, 0)

    messages.land()

    def joined(pick):
        return jnp.concatenate([pick(t) for t in range(C)], axis=1)

    def places(pick):
        code = joined(pick).astype(jnp.int32)
        return divide(code, BC * C), remainder(code, BC)

    place_r = iota((BR, S), 0)
    place_c = iota((BC, S), 0)

    def one_hot(hit):
        return jnp.where(hit, 1.0, 0.0).astype(BF16)

    in_row, in_col = places(lambda t: msg_row[t, 1, 0:1, :])
    in_weight = joined(lambda t: msg_row[t, 1, 1:2, :])
    row_hit = place_r == in_row
    col_hot = one_hot(place_c == in_col)
    hot_own[...] = col_hot
    hi, lo = halves(cinit[0])
    seen = dot(hi, col_hot) + dot(lo, col_hot)
    at_via = jnp.sum(jnp.where(row_hit, seen, 0.0), axis=0, keepdims=True)
    for t in range(C):
        val_out[t] = at_via[:, t * per : (t + 1) * per]
    val_in[col] = val_out[col]
    values = Batch(always, always, val_in.at[pl.ds(0, C - 1)], [
        (val_out.at[lax.rem(col + d, C)], val_in.at[col], (row, lax.rem(col + d, C)))
        for d in range(1, C)
    ])

    messages_up = Batch(top_ok, bot_ok, msg_ud.at[1], [
        (msg_out.at[lax.rem(col + d, C) + 1], msg_ud.at[1, col], (up, lax.rem(col + d, C)))
        for d in range(C)
    ])
    messages_down = Batch(bot_ok, top_ok, msg_ud.at[0], [
        (msg_out.at[lax.rem(col + d, C) + 1], msg_ud.at[0, col], (down, lax.rem(col + d, C)))
        for d in range(C)
    ])

    dinv_corners = corner_send(0)

    cleak_load.wait()
    only = jnp.where(row_hit, in_weight, 0.0).astype(BF16)
    coarse_diag = 4.0 * coarse_conductance + cleak[...] + dot_t(only, col_hot)
    scale = relaxation / coarse_diag
    coarse_land(coarse0, 0, 1)
    volt = cinit[0]
    sides = beside(turn.at[0], R, C, volt, crow_top[0, 7:8, :], crow_bot[0, 0:1, :], cleft[0], cright[0])
    coarse[0] = volt + scale * (coarse_conductance * sides - coarse_diag * volt)
    coarse[1] = scale
    coarse[2] = coarse_diag
    for n in range(2):
        seams(coarse[n], n + 1)
    coarse_later = coarse_send(coarse.at[pl.ds(0, 2)], 1, 2)

    def quiet(ref, shape):
        def body():
            for t in range(C):
                ref[t] = jnp.zeros(shape, F32)
        return body

    left_row, left_col = places(lambda t: msg_row[t, 0, 0:1, :])
    right_row, right_col = places(lambda t: msg_row[t, 2, 0:1, :])
    hot_left[...] = one_hot(place_r == left_row)
    hot_right[...] = one_hot(place_r == right_row)

    def edge_copy(F, X, size):
        X[...] = edges_of(F[0:TR, :], F[(NB - 1) * size : (NB - 1) * size + TR, :], None)

    edge_copy(D, Dq, TR)
    halo_land(dv, dvq, 0, dinv_copies)

    for copy in amp_loads:
        copy.wait()
    values.land()
    drops = weight * joined(lambda o: val_in[o])
    drop_hi, drop_lo = halves(drops)
    half_step = TR

    def inject(i, carry):
        at = pl.ds(pl.multiple_of(i * half_step, half_step), half_step)
        hot = row_hot[at, :]
        added = dot(hot * drop_hi, Bt[...]) + dot(hot * drop_lo, Bt[...])
        for b in range(NB):
            inner = pl.ds(pl.multiple_of(b * EXT + PAD + i * half_step, 8), half_step)
            own = pl.ds(pl.multiple_of(b * TR + i * half_step, 8), half_step)
            value = amp[b, at, :] * mask[b, at, :].astype(F32) + added[:, b * LANES : (b + 1) * LANES]
            rhs[own, :] = value
            value = value * dv[inner, :]
            V[0, inner, :] = value
            woven[pl.ds((b * TR + i * half_step) * ITERS, half_step, stride=ITERS), :] = value
        return carry

    lax.fori_loop(0, TR // half_step, inject, 0)
    first_copies = halo_send(V.at[0], 1)
    corner_land(dvq, 0, dinv_corners)
    first_corners = corner_send(1)
    edge_copy(rhs, rhsq, TR)

    def stencil(k, start, size):
        place = wide(size)
        mids = [V[k, pl.ds(b * EXT + start, size), :] for b in range(NB)]
        lefts = [pltpu.roll(m, 1, 1) for m in mids]
        rights = [pltpu.roll(m, LANES - 1, 1) for m in mids]
        out = []
        for b in range(NB):
            tall = V[k, pl.ds(b * EXT + start - 1, size), :] + V[k, pl.ds(b * EXT + start + 1, size), :]
            before = jnp.where(place == 0, lefts[b - 1], lefts[b])
            after = jnp.where(place == LANES - 1, rights[(b + 1) % NB], rights[b])
            out.append(tall + (before + after))
        return mids, out

    def inward(b, value):
        place = wide(value.shape[0])
        if b == 0:
            value = jnp.where(place >= EDGE, value, 0.0)
        if b == NB - 1:
            value = jnp.where(place < LANES - EDGE, value, 0.0)
        return value

    def advance(k, start, size, totals, start0=None):
        start0 = start if start0 is None else start0
        mids, near = stencil(k, start, size)
        totals = None if totals is None else list(totals)
        for b in range(NB):
            at = pl.ds(b * EXT + start, size)
            own = pl.ds(b * TR + start - PAD, size)
            if k < ITERS - 1:
                fresh = dv[at, :] * near[b]
                if k:
                    fresh = (fresh + fresh) - V[k - 1, at, :]
                V[k + 1, at, :] = fresh
                if PAD <= start0 < PAD + TR:
                    woven[pl.ds((b * TR + start - PAD) * ITERS + k + 1, size, stride=ITERS), :] = fresh
                if totals is None:
                    continue
                if k == 0:
                    right_side = rhs[own, :]
                    applied = inward(b, right_side - near[b])
                    R0[own, :] = applied
                    totals[0] = totals[0] + fold(right_side * mids[b])
                    totals[1] = totals[1] + fold(applied * mids[b])
                    totals[2] = totals[2] + fold(applied * fresh)
                else:
                    totals[0] = totals[0] + fold(R0[own, :] * fresh)
            elif totals is not None:
                applied = inward(b, D[own, :] * mids[b] - near[b])
                totals[ITERS - 2] = totals[ITERS - 2] + fold(applied * mids[b])
                for j in range(1, ITERS - 1):
                    totals[j - 1] = totals[j - 1] + fold(applied * V[j, at, :])
        return None if totals is None else tuple(totals)

    def blank(n):
        return tuple(jnp.zeros((8, LANES), F32) for _ in range(n))

    kept = [3] + [1] * (ITERS - 2) + [ITERS - 1]
    inside = TR - 2 * EDGE
    chunk = inside // 2 if inside % 16 == 0 else inside
    piece = 8
    sums = []
    for k in range(ITERS):
        if k < ITERS - 1:
            advance(k, PAD, EDGE, None)
            advance(k, PAD + TR - EDGE, EDGE, None)

        def body(i, carry, k=k):
            for at in range(0, chunk, piece):
                carry = advance(k, PAD + EDGE + i * chunk + at, min(piece, chunk - at), carry, PAD)
            return carry

        sums.append(lax.fori_loop(0, inside // chunk, body, blank(kept[k])))

    halo_land(V.at[0], Q.at[0], 1, first_copies)
    corner_land(Q.at[0], 1, first_corners)
    def rim(value):
        place = wide(value.shape[0])
        ours = (place < EDGE) | ((place >= HALF - EDGE) & (place < HALF))
        return jnp.where(ours, value, 0.0)

    def advance_edge(k, start, size, totals):
        mid = Q[k, pl.ds(start, size), :]
        near = Q[k, pl.ds(start - 1, size), :] + Q[k, pl.ds(start + 1, size), :]
        near = near + (pltpu.roll(mid, 1, 1) + pltpu.roll(mid, LANES - 1, 1))
        at = pl.ds(start, size)
        own = pl.ds(start - PAD, size)
        totals = None if totals is None else list(totals)
        if k < ITERS - 1:
            fresh = dvq[at, :] * near
            if k:
                fresh = (fresh + fresh) - Q[k - 1, at, :]
            Q[k + 1, at, :] = fresh
            if totals is not None:
                place = wide(size)
                value = jnp.where(place < EDGE, fresh, V[k + 1, at, :])
                V[k + 1, at, :] = value
                woven[pl.ds((start - PAD) * ITERS + k + 1, size, stride=ITERS), :] = value
                far = pl.ds(last + start, size)
                value = jnp.where(place >= LANES - EDGE, pltpu.roll(fresh, HALF, 1), V[k + 1, far, :])
                V[k + 1, far, :] = value
                woven[pl.ds(((NB - 1) * TR + start - PAD) * ITERS + k + 1, size, stride=ITERS), :] = value
                if k == 0:
                    applied = rim(rhsq[own, :] - near)
                    rhsq[own, :] = applied
                    totals[1] = totals[1] + fold(applied * mid)
                    totals[2] = totals[2] + fold(applied * fresh)
                else:
                    totals[0] = totals[0] + fold(rhsq[own, :] * fresh)
        elif totals is not None:
            applied = rim(Dq[own, :] * mid - near)
            totals[ITERS - 2] = totals[ITERS - 2] + fold(applied * mid)
            for j in range(1, ITERS - 1):
                totals[j - 1] = totals[j - 1] + fold(applied * Q[j, at, :])
        return None if totals is None else tuple(totals)

    for k in range(ITERS):
        if k < ITERS - 1:
            advance(k, PAD - EDGE, EDGE, None)
            advance(k, PAD + TR, EDGE, None)
            advance_edge(k, PAD - EDGE, EDGE, None)
            advance_edge(k, PAD + TR, EDGE, None)
        sums[k] = advance(k, PAD, EDGE, sums[k])
        sums[k] = advance(k, PAD + TR - EDGE, EDGE, sums[k])
        sums[k] = advance_edge(k, PAD, TR, sums[k])

    flat = [total for part in sums for total in part]
    tile = jnp.concatenate([jnp.sum(total, axis=0, keepdims=True) for total in flat], axis=0)
    sub = iota((8, LANES), 0)
    number = len(flat)
    tile = jnp.sum(tile, axis=1, keepdims=True)
    red_out[...] = jnp.sum(jnp.where(sub == lane_row, tile, 0.0), axis=0, keepdims=True)
    me = row * C + col
    early = len(pending)
    red_in[me] = red_out[...]
    reductions = Batch(always, always, red_in.at[pl.ds(0, R * C - 1)], [
        (red_out, red_in.at[me], (lax.rem(row + e, R), lax.rem(col + d, C)))
        for e in reversed(range(R)) for d in reversed(range(C)) if e or d
    ])

    spot_copy.wait()
    unroll = 32

    def pick(i, carry):
        for n in range(unroll):
            s = i * unroll + n
            where = spot[0, s]
            picked[pl.ds(pl.multiple_of(s * ITERS, ITERS), ITERS), :] = woven[pl.ds(where, ITERS), :]
        return carry

    lax.fori_loop(0, S // unroll, pick, 0)
    diag_hit = iota((per, LANES), 0) == iota((per, LANES), 1)

    for o in range(C):
        part = slice(o * per, (o + 1) * per)
        hot = lane_hot[part, :]
        for k in range(ITERS):
            mine = picked[pl.ds(o * per * ITERS + k, per, stride=ITERS), :]
            value = jnp.sum(mine * hot, axis=1, keepdims=True)
            seen_out[o + 1, k : k + 1, :] = jnp.sum(jnp.where(diag_hit, value, 0.0), axis=0, keepdims=True)
    seen_out[0] = seen_out[C]
    seen_out[C + 1] = seen_out[1]
    seen_row[col] = seen_out[pl.ds(col, 3)]
    seen_side = Batch(always, always, seen_row.at[pl.ds(0, C - 1)], [
        (seen_out.at[pl.ds(lax.rem(col + d, C), 3)], seen_row.at[col], (row, lax.rem(col + d, C)))
        for d in range(1, C)
    ])
    seen_up = Batch(top_ok, bot_ok, seen_ud.at[1], [
        (seen_out.at[lax.rem(col + d, C) + 1], seen_ud.at[1, col], (up, lax.rem(col + d, C)))
        for d in range(C)
    ])
    seen_down = Batch(bot_ok, top_ok, seen_ud.at[0], [
        (seen_out.at[lax.rem(col + d, C) + 1], seen_ud.at[0, col], (down, lax.rem(col + d, C)))
        for d in range(C)
    ])

    messages_down.land(quiet(msg_ud.at[0], (2, per)))
    messages_up.land(quiet(msg_ud.at[1], (2, per)))
    above_row, above_col = places(lambda t: msg_ud[0, t, 0:1, :])
    below_row, below_col = places(lambda t: msg_ud[1, t, 0:1, :])
    hot_up[...] = one_hot(place_c == above_col)
    hot_down[...] = one_hot(place_c == below_col)


    coarse_land(coarse_later, 1, 2)
    beyond_rows[0] = crow_top[1:3]
    beyond_rows[1] = crow_bot[1:3]
    beyond_cols[0] = cleft[1:3]
    beyond_cols[1] = cright[1:3]
    own_row, own_col = places(lambda t: msg_row[t, 1, 0:1, :])
    for n, part in enumerate((own_row, left_col, right_col, above_row, below_row)):
        nodes[n : n + 1, :] = part
    seen_side.land()
    seen_down.land(quiet(seen_ud.at[0], (ITERS, per)))
    seen_up.land(quiet(seen_ud.at[1], (ITERS, per)))
    heard = (
        (lambda t: seen_row[t, 1], lambda t: msg_row[t, 1, 1:2, :]),
        (lambda t: seen_row[t, 0], lambda t: msg_row[t, 0, 1:2, :]),
        (lambda t: seen_row[t, 2], lambda t: msg_row[t, 2, 1:2, :]),
        (lambda t: seen_ud[0, t], lambda t: msg_ud[0, t, 1:2, :]),
        (lambda t: seen_ud[1, t], lambda t: msg_ud[1, t, 1:2, :]),
    )
    for n, (seen, weights) in enumerate(heard):
        for t in range(C):
            basis[n, :, t * per : (t + 1) * per] = seen(t) * weights(t)

    for batch in pending[:early]:
        batch.leave()
    reductions.land()
    parts = [red_in[n] for n in range(R * C)]
    while len(parts) > 1:
        parts = [sum(parts[n : n + 2][1:], parts[n]) for n in range(0, len(parts), 2)]
    total = jnp.broadcast_to(parts[0], (8, LANES))
    total = jnp.sum(jnp.where(sub == lane_row, total, 0.0), axis=1, keepdims=True)
    scalar = [total[n : n + 1, :] for n in range(number)]
    energy = [scalar[1], scalar[2]] + scalar[3 : 3 + ITERS - 2]
    high = scalar[3 + ITERS - 2 :]
    for j in range(1, ITERS):
        energy.append(2.0 * high[j - 1] - energy[ITERS - 1 - j])
    moment = [scalar[0], scalar[0] - energy[0]]
    for n in range(2, ITERS):
        moment.append(2.0 * (moment[n - 1] - energy[n - 1]) - moment[n - 2])
    matrix = [[None] * (ITERS + 1) for _ in range(ITERS)]
    for j in range(ITERS):
        for k in range(j + 1):
            matrix[j][k] = matrix[k][j] = 0.5 * (energy[j + k] + energy[j - k])
        matrix[j][ITERS] = moment[j]
    for i in range(ITERS):
        inverse = 1.0 / matrix[i][i]
        for k in range(i + 1, ITERS + 1):
            matrix[i][k] = matrix[i][k] * inverse
        for j in range(i + 1, ITERS):
            for k in range(i + 1, ITERS + 1):
                matrix[j][k] = matrix[j][k] - matrix[j][i] * matrix[i][k]
    coef = [None] * ITERS
    for i in reversed(range(ITERS)):
        coef[i] = matrix[i][ITERS]
        for k in range(i + 1, ITERS):
            coef[i] = coef[i] - matrix[i][k] * coef[k]
    for k in range(ITERS):
        coef[k] = jnp.broadcast_to(coef[k], (1, LANES))
        coef_out[k : k + 1, :] = coef[k]
    for at in range(0, TR, 8):
        for b in range(NB):
            inner = pl.ds(b * EXT + PAD + at, 8)
            value = coef[0] * V[0, inner, :]
            for k in range(1, ITERS):
                value = value + coef[k] * V[k, inner, :]
            x_out[at : at + 8, b * LANES : (b + 1) * LANES] = value
    assert count[0] == send_sem.shape[0]
    for batch in pending[early:]:
        batch.leave()


def finish(
    R, C, x, coef, nodes, basis, coarse, beyond_rows, beyond_cols,
    hot_own, hot_left, hot_right, hot_up, hot_down,
    x_out, c_out, c, turn, sem,
):
    store = pltpu.make_async_copy(x, x_out, sem.at[0])
    store.start()
    BR, BC = c.shape
    S = basis.shape[2]
    groups = BC // GROUP
    by = [jnp.concatenate([coef[k : k + 1, :]] * (S // LANES), axis=1) for k in range(ITERS)]

    def gathered(n, hit, hot):
        amount = by[0] * basis[n, 0:1, :]
        for k in range(1, ITERS):
            amount = amount + by[k] * basis[n, k : k + 1, :]
        out = dot_t(spread(hit, amount), hot[...])
        return out[: out.shape[0] // 2] + out[out.shape[0] // 2 :]

    place_g = iota((groups, S), 0) * GROUP
    one_row = iota((8, S), 0) == 0
    on_left = gathered(1, place_g + (GROUP - 1) == nodes[1:2, :], hot_left)
    on_right = gathered(2, place_g == nodes[2:3, :], hot_right)
    on_above = gathered(3, one_row & (nodes[3:4, :] == BR - 1), hot_up)
    on_below = gathered(4, one_row & (nodes[4:5, :] == 0), hot_down)
    sources = gathered(0, iota((BR, S), 0) == nodes[0:1, :], hot_own)
    scale = coarse[1]
    volt = coarse[0] + scale * sources
    sides = beside(
        turn, R, C, volt,
        beyond_rows[0, 0, 7:8, :] + beyond_rows[0, 1, 7:8, :] * on_above[0:1, :],
        beyond_rows[1, 0, 0:1, :] + beyond_rows[1, 1, 0:1, :] * on_below[0:1, :],
        beyond_cols[0, 0] + beyond_cols[0, 1] * on_left,
        beyond_cols[1, 0] + beyond_cols[1, 1] * on_right,
    )
    c[...] = volt + scale * (sources + coarse_conductance * sides - coarse[2] * volt)
    last = pltpu.make_async_copy(c, c_out, sem.at[1])
    last.start()
    store.wait()
    last.wait()


def per_device(R, C, load_amp, load_mask, leak, coarse_leak, coarse_init, via_fine, via_coarse, via_count):
    inputs = (load_amp, load_mask, leak, coarse_leak, coarse_init, via_fine, via_coarse, via_count)
    TR, TC = leak.shape
    BR, BC = coarse_leak.shape
    S = via_fine.shape[1]
    per = S // C
    NB = TC // LANES
    EXT = TR + 2 * PAD
    groups = BC // GROUP
    batches = 24
    vmem = pl.BlockSpec(memory_space=pltpu.VMEM)
    state = pl.pallas_call(
        functools.partial(kernel, R, C),
        out_shape=(
            pltpu.VMEM((TR, TC), F32), pltpu.VMEM((8, LANES), F32), pltpu.VMEM((8, S), jnp.int32),
            pltpu.VMEM((5, ITERS, S), F32), pltpu.VMEM((3, BR, BC), F32),
            pltpu.VMEM((2, 2, 8, BC), F32), pltpu.VMEM((2, 2, groups, BR), F32),
            pltpu.VMEM((BC, S), BF16), pltpu.VMEM((BR, S), BF16), pltpu.VMEM((BR, S), BF16),
            pltpu.VMEM((BC, S), BF16), pltpu.VMEM((BC, S), BF16),
        ),
        in_specs=[pl.BlockSpec(memory_space=pltpu.HBM)] * 8,
        out_specs=(vmem,) * 12,
        scratch_shapes=[
            pltpu.VMEM((NB, TR, LANES), F32), pltpu.VMEM((NB, TR, LANES), jnp.int32),
            pltpu.VMEM((NB, TR, LANES), F32),
            pltpu.VMEM((BR, BC), F32), pltpu.VMEM((1, BR, BC), F32),
            pltpu.VMEM((1, S), jnp.int32), pltpu.VMEM((1, S), jnp.int32),
            pltpu.SMEM((1, C), jnp.int32), pltpu.SemaphoreType.DMA((9,)),
            pltpu.VMEM((C + 2, 2, per), F32), pltpu.VMEM((C, 3, 2, per), F32), pltpu.VMEM((2, C, 2, per), F32),
            pltpu.VMEM((C, 1, per), F32), pltpu.VMEM((C, 1, per), F32),
            pltpu.VMEM((C + 2, ITERS, per), F32), pltpu.VMEM((C, 3, ITERS, per), F32),
            pltpu.VMEM((2, C, ITERS, per), F32),
            pltpu.VMEM((1, S), jnp.int32), pltpu.SMEM((1, S), jnp.int32),
            pltpu.VMEM((NB * TR * ITERS, LANES), F32),
            pltpu.VMEM((ITERS * S, LANES), F32), pltpu.VMEM((S, LANES), F32),
            pltpu.VMEM((TR, S), BF16),
            pltpu.VMEM((S, TC), BF16),
            pltpu.VMEM((NB * EXT, LANES), F32),
            pltpu.VMEM((NB * TR, LANES), F32),
            pltpu.VMEM((EXT, LANES), F32),
            pltpu.VMEM((TR, LANES), F32),
            pltpu.VMEM((ITERS, NB * EXT, LANES), F32),
            pltpu.VMEM((ITERS, EXT, LANES), F32),
            pltpu.VMEM((NB * TR, LANES), F32),
            pltpu.VMEM((NB * TR, LANES), F32),
            pltpu.VMEM((TR, LANES), F32),
            pltpu.VMEM((2, TR, LANES), F32),
            pltpu.VMEM((2, LANES, TR), F32),
            pltpu.VMEM((2, LANES, TR), F32),
            pltpu.VMEM((2, NB, EDGE, LANES), F32),
            pltpu.VMEM((2, NB, EDGE, LANES), F32),
            pltpu.VMEM((2, 4, EDGE, LANES), F32),
            pltpu.VMEM((1, LANES), F32), pltpu.VMEM((R * C, 1, LANES), F32),
            pltpu.VMEM((3, BC, BR), F32), pltpu.VMEM((3, 2, groups, BR), F32),
            pltpu.VMEM((3, 8, BC), F32), pltpu.VMEM((3, 8, BC), F32),
            pltpu.VMEM((3, groups, BR), F32), pltpu.VMEM((3, groups, BR), F32),
            pltpu.SemaphoreType.DMA((batches,)),
            pltpu.SemaphoreType.DMA((batches,)),
        ],
        compiler_params=pltpu.CompilerParams(
            collective_id=0, has_side_effects=True, vmem_limit_bytes=40000 * 1024
        ),
    )(*(pltpu.with_memory_space_constraint(v, pltpu.HBM) for v in inputs))
    return pl.pallas_call(
        functools.partial(finish, R, C),
        out_shape=(jax.ShapeDtypeStruct((TR, TC), F32), jax.ShapeDtypeStruct((BR, BC), F32)),
        in_specs=[vmem] * 12,
        out_specs=(pl.BlockSpec(memory_space=pltpu.HBM),) * 2,
        scratch_shapes=[
            pltpu.VMEM((BR, BC), F32), pltpu.VMEM((BC, BR), F32), pltpu.SemaphoreType.DMA((2,)),
        ],
        compiler_params=pltpu.CompilerParams(vmem_limit_bytes=16000 * 1024),
    )(*(pltpu.with_memory_space_constraint(v, pltpu.VMEM) for v in state))


def solution(mesh):
    spec = P("row", "col")
    return jax.shard_map(
        functools.partial(per_device, mesh.shape["row"], mesh.shape["col"]),
        mesh=mesh, in_specs=(spec,) * 8, out_specs=(spec, spec), check_vma=False,
    )
```

```python
import functools
import jax
import jax.numpy as jnp
from jax import lax
from jax.experimental import pallas as pl
from jax.experimental.pallas import tpu as pltpu
from jax.sharding import PartitionSpec as P

GROUP = 16
ITERS = 4
LANES = 128
PAD = 16
EDGE = 8
HALF = LANES // 2
QUARTER = LANES // 4

via_conductance = 2.0
coarse_conductance = 4.0
relaxation = 0.8

F32 = jnp.float32
BF16 = jnp.bfloat16
MESH = pl.DeviceIdType.MESH


def divide(value, by):
    if by & (by - 1) == 0:
        return lax.shift_right_logical(value, by.bit_length() - 1)
    return value // by


def remainder(value, by):
    if by & (by - 1) == 0:
        return value & (by - 1)
    return value % by


def halves(value):
    high = value.astype(BF16).astype(F32)
    return high.astype(BF16), (value - high).astype(BF16)


def dot(a, b):
    return jnp.dot(a, b, preferred_element_type=F32)


def dot_t(a, b):
    return lax.dot_general(a, b, (((1,), (1,)), ((), ())), preferred_element_type=F32)


def fold(value):
    total = value[0:8]
    for n in range(1, value.shape[0] // 8):
        total = total + value[n * 8 : (n + 1) * 8]
    return total


def iota(shape, dim):
    return lax.broadcasted_iota(jnp.int32, shape, dim)


def spread(hit, amount):
    hi, lo = halves(amount)
    zero = jnp.zeros((), BF16)
    return jnp.concatenate([jnp.where(hit, hi, zero), jnp.where(hit, lo, zero)], axis=0)


def beside(turn, R, C, volt, above, below, far_left, far_right):
    row, col = lax.axis_index("row"), lax.axis_index("col")
    BR, BC = volt.shape
    groups = BC // GROUP
    place_v = iota((BR, BC), 0)
    within = remainder(iota((BR, BC), 1), GROUP)
    group = iota((groups, BR), 0)
    above = jnp.where(place_v == 0, jnp.where(row > 0, above, 0.0), pltpu.roll(volt, 1, 0))
    below = jnp.where(place_v == BR - 1, jnp.where(row < R - 1, below, 0.0), pltpu.roll(volt, BR - 1, 0))
    turn[pl.ds(0, groups, stride=GROUP), :] = jnp.where(
        col > 0, far_left, jnp.where(group == 0, 0.0, jnp.roll(far_left, 1, 0))
    )
    turn[pl.ds(GROUP - 1, groups, stride=GROUP), :] = jnp.where(
        col < C - 1, far_right, jnp.where(group == groups - 1, 0.0, jnp.roll(far_right, -1, 0))
    )
    edge = turn[...].T
    before = jnp.where(within == 0, edge, pltpu.roll(volt, 1, 1))
    after = jnp.where(within == GROUP - 1, edge, pltpu.roll(volt, BC - 1, 1))
    return above + below + before + after


def kernel(
    R, C,
    amp_in, mask_in, leak_in, cleak_in, cinit_in, vf_in, vc_in, cnt_in,
    x_out, coef_out, nodes, basis, coarse, beyond_rows, beyond_cols,
    hot_own, hot_left, hot_right, hot_up, hot_down,
    amp, mask, leak, cleak, cinit, vf, vc, cnt, load_sem,
    msg_out, msg_row, msg_ud, val_out, val_in, seen_out, seen_row, seen_ud,
    spot_v, spot, woven, picked, lane_hot,
    row_hot, Bt, dv, D, dvq, Dq, V, Q, R0, rhs, rhsq,
    E, ET, H, rtop, rbot, rcorner,
    red_out, red_in,
    turn, seam_out, crow_top, crow_bot, cleft, cright,
    send_sem, recv_sem,
):
    row, col = lax.axis_index("row"), lax.axis_index("col")
    TR, TC = leak_in.shape
    NB = TC // LANES
    EXT = TR + 2 * PAD
    BR, BC = cleak.shape
    S = vf.shape[1]
    per = S // C
    groups = BC // GROUP

    def cut(b):
        return pl.ds(b * LANES, LANES)

    loads = []

    def load(source, target):
        copy = pltpu.make_async_copy(source, target, load_sem.at[len(loads)])
        copy.start()
        loads.append(copy)
        return copy

    def load_blocks(source, target):
        sem = load_sem.at[len(loads)]
        for b in range(NB):
            pltpu.make_async_copy(source.at[:, cut(b)], target.at[b], sem).start()
        copy = pltpu.make_async_copy(target, target, sem)
        loads.append(copy)
        return copy

    small = [load(cnt_in, cnt), load(vc_in, vc), load(vf_in, vf)]
    cinit_load = load(cinit_in, cinit.at[0])
    leak_load = load_blocks(leak_in, leak)
    cleak_load = load(cleak_in, cleak)
    amp_loads = [load_blocks(amp_in, amp), load_blocks(mask_in, mask)]

    up, down = lax.rem(row + R - 1, R), lax.rem(row + 1, R)
    left, right = lax.rem(col + C - 1, C), lax.rem(col + 1, C)
    top_ok, bot_ok = row > 0, row < R - 1
    left_ok, right_ok = col > 0, col < C - 1
    always = None

    barrier = pltpu.get_barrier_semaphore()

    def greet(r, c):
        pl.semaphore_signal(barrier, inc=1, device_id=(r, c), device_id_type=MESH)

    for d in range(1, C):
        greet(row, lax.rem(col + d, C))
    near_rows = R <= 4
    if near_rows:

        @pl.when(top_ok)
        def _():
            greet(up, col)

        @pl.when(bot_ok)
        def _():
            greet(down, col)
    else:
        for e in range(1, R):
            for d in range(C):
                greet(lax.rem(row + e, R), lax.rem(col + d, C))

    def welcome():
        if near_rows:
            rows = jnp.where(top_ok, 1, 0) + jnp.where(bot_ok, 1, 0)
            pl.semaphore_wait(barrier, C - 1 + rows)
        else:
            pl.semaphore_wait(barrier, R * C - 1)

    count = [0]
    pending = []

    def under(ok, body):
        if ok is always:
            body()
        else:
            pl.when(ok)(body)

    class Batch:
        def __init__(self, ok, heard, whole, specs):
            self.ok, self.heard = ok, heard
            n = count[0]
            count[0] += 1

            def make(src, dst, device):
                return pltpu.make_async_remote_copy(
                    src_ref=src, dst_ref=dst, send_sem=send_sem.at[n], recv_sem=recv_sem.at[n],
                    device_id=device, device_id_type=MESH,
                )

            self.all = make(whole, whole, specs[0][2])
            pending.append(self)

            def start():
                for spec in specs:
                    make(*spec).start()

            under(ok, start)

        def land(self, otherwise=None):
            under(self.heard, self.all.wait_recv)
            if self.heard is not always and otherwise is not None:
                pl.when(jnp.logical_not(self.heard))(otherwise)

        def leave(self):
            under(self.ok, self.all.wait_send)

    for copy in small:
        copy.wait()
    lane = iota((1, per), 1)
    weight = jnp.concatenate(
        [jnp.where(lane < cnt[0, o], via_conductance, 0.0).astype(F32) for o in range(C)], axis=1
    )
    node = vc[...].astype(F32)
    for o in [-1] + list(range(C)) + [C]:
        part = slice((o % C) * per, (o % C + 1) * per)
        msg_out[o + 1, 0:1, :] = node[:, part]
        msg_out[o + 1, 1:2, :] = weight[:, part]
    msg_row[col] = msg_out[pl.ds(col, 3)]
    fine = vf[...]
    fine_row = divide(fine, TC)
    fine_col = remainder(fine, TC)
    spot_v[...] = (divide(fine_col, LANES) * TR + fine_row) * ITERS
    spot_copy = pltpu.make_async_copy(spot_v, spot, load_sem.at[len(loads)])
    spot_copy.start()
    step = 64

    def build_rows(i, carry):
        at = pl.ds(pl.multiple_of(i * step, step), step)
        place = iota((step, S), 0) + i * step
        row_hot[at, :] = jnp.where(place == fine_row, 1.0, 0.0).astype(BF16)
        return carry

    lax.fori_loop(0, TR // step, build_rows, 0)

    welcome()

    messages = Batch(always, always, msg_row.at[pl.ds(0, C - 1)], [
        (msg_out.at[pl.ds(lax.rem(col + d, C), 3)], msg_row.at[col], (row, lax.rem(col + d, C)))
        for d in range(1, C)
    ])

    def seams(volt, n):
        turn[n] = volt.T
        seam_out[n, 0] = turn[n, pl.ds(0, groups, stride=GROUP), :]
        seam_out[n, 1] = turn[n, pl.ds(GROUP - 1, groups, stride=GROUP), :]

    def coarse_send(rows, n, m):
        at = pl.ds(n, m)
        return [
            Batch(top_ok, bot_ok, crow_bot.at[at], [(rows.at[:, pl.ds(0, 8)], crow_bot.at[at], (up, col))]),
            Batch(bot_ok, top_ok, crow_top.at[at], [(rows.at[:, pl.ds(BR - 8, 8)], crow_top.at[at], (down, col))]),
            Batch(always, always, seam_out.at[at], [
                (seam_out.at[at, 0], cright.at[at], (row, left)),
                (seam_out.at[at, 1], cleft.at[at], (row, right)),
            ]),
        ]

    def coarse_land(batches, n, m):
        def no_below():
            crow_bot[n : n + m] = jnp.zeros((m, 8, BC), F32)

        def no_above():
            crow_top[n : n + m] = jnp.zeros((m, 8, BC), F32)

        batches[0].land(no_below)
        batches[1].land(no_above)
        batches[2].land()

    cinit_load.wait()
    seams(cinit[0], 0)
    coarse0 = coarse_send(cinit, 0, 1)
    lanes = iota((per, LANES), 1).astype(F32)
    for o in range(C):
        part = slice(o * per, (o + 1) * per)
        turned = jnp.broadcast_to(fine_col[:, part].astype(F32), (LANES, per)).T
        near = turned
        total = jnp.zeros((per, LANES), F32)
        for b in range(NB):
            hot = jnp.where(turned == lanes + b * LANES, 1.0, 0.0)
            Bt[part, b * LANES : (b + 1) * LANES] = hot.astype(BF16)
            total = total + hot
        lane_hot[part, :] = total

    zero_pad = jnp.zeros((8, LANES), F32)
    for n in range(ITERS):
        for b in range(NB):
            V[n, b * EXT : b * EXT + 8, :] = zero_pad
            V[n, (b + 1) * EXT - 8 : (b + 1) * EXT, :] = zero_pad
        for b in range(NB if n == 0 else 0):
            V[n, b * EXT + 8 : b * EXT + 16, :] = zero_pad
            V[n, (b + 1) * EXT - 16 : (b + 1) * EXT - 8, :] = zero_pad
        Q[n, 0:8, :] = zero_pad
        Q[n, EXT - 8 : EXT, :] = zero_pad
    for n in range(1, ITERS):
        for b in range(NB):
            V[n, b * EXT + 8 : b * EXT + 16, :] = zero_pad
            V[n, (b + 1) * EXT - 16 : (b + 1) * EXT - 8, :] = zero_pad

    leak_load.wait()
    wide_step = 256 if TR % 256 == 0 else step
    weight_low = weight.astype(BF16)

    def diagonal(i, carry):
        at = pl.ds(pl.multiple_of(i * wide_step, wide_step), wide_step)
        sums = dot(row_hot[at, :] * weight_low, Bt[...])
        for b in range(NB):
            inner = pl.ds(pl.multiple_of(b * EXT + PAD + i * wide_step, 8), wide_step)
            own = pl.ds(pl.multiple_of(b * TR + i * wide_step, 8), wide_step)
            value = 4.0 + leak[b, at, :] + sums[:, b * LANES : (b + 1) * LANES]
            D[own, :] = value
            dv[inner, :] = 1.0 / value
        return carry

    lax.fori_loop(0, TR // wide_step, diagonal, 0)

    lane_row = iota((8, LANES), 1)

    def wide(rows):
        return iota((rows, LANES), 1)

    def keep(ok, value):
        return value * jnp.where(ok, 1.0, 0.0).astype(F32)

    last = (NB - 1) * EXT

    def halo_send(F, n):
        edge = jnp.where(wide(TR) < HALF, F[PAD : PAD + TR, :], F[last + PAD : last + PAD + TR, :])
        E[n] = edge
        ET[n] = edge.T
        sides = Batch(always, always, ET.at[n, pl.ds(0, 2 * EDGE)], [
            (ET.at[n, pl.ds(0, EDGE)], H.at[n, pl.ds(HALF, EDGE)], (row, left)),
            (ET.at[n, pl.ds(LANES - EDGE, EDGE)], H.at[n, pl.ds(LANES - EDGE, EDGE)], (row, right)),
        ])
        above = Batch(top_ok, bot_ok, rbot.at[n], [
            (F.at[pl.ds(b * EXT + PAD, EDGE)], rbot.at[n, b], (up, col)) for b in range(NB)
        ])
        below = Batch(bot_ok, top_ok, rtop.at[n], [
            (F.at[pl.ds(b * EXT + PAD + TR - EDGE, EDGE)], rtop.at[n, b], (down, col)) for b in range(NB)
        ])
        return sides, above, below

    def corner_send(n):
        above = Batch(top_ok, bot_ok, rcorner.at[n, pl.ds(2, 2)], [
            (E.at[n, pl.ds(0, EDGE)], rcorner.at[n, 3], (up, left)),
            (E.at[n, pl.ds(0, EDGE)], rcorner.at[n, 2], (up, right)),
        ])
        below = Batch(bot_ok, top_ok, rcorner.at[n, pl.ds(0, 2)], [
            (E.at[n, pl.ds(TR - EDGE, EDGE)], rcorner.at[n, 1], (down, left)),
            (E.at[n, pl.ds(TR - EDGE, EDGE)], rcorner.at[n, 0], (down, right)),
        ])
        return above, below

    def edges_of(first, final, beyond):
        rows = first.shape[0]
        place = wide(rows)
        own = jnp.where(place < QUARTER, first, pltpu.roll(final, HALF, 1))
        if beyond is None:
            return own
        return jnp.where(place < HALF, own, beyond)

    def outer(right_side, left_side):
        place = wide(right_side.shape[0])
        right_side = jnp.where((place < HALF + EDGE) & right_ok, right_side, 0.0)
        return jnp.where((place >= LANES - EDGE) & left_ok, left_side, right_side)

    def halo_land(F, X, n, batches):
        sides, above, below = batches
        sides.land()
        side = H[n].T
        X[PAD : PAD + TR, :] = edges_of(
            F[PAD : PAD + TR, :], F[last + PAD : last + PAD + TR, :], outer(side, side)
        )

        def no_below():
            for b in range(NB):
                F[b * EXT + PAD + TR : b * EXT + PAD + TR + EDGE, :] = zero_pad

        def no_above():
            for b in range(NB):
                F[b * EXT + PAD - EDGE : b * EXT + PAD, :] = zero_pad

        above.land(no_below)
        below.land(no_above)

        @pl.when(bot_ok)
        def _():
            for b in range(NB):
                F[b * EXT + PAD + TR : b * EXT + PAD + TR + EDGE, :] = rbot[n, b]

        @pl.when(top_ok)
        def _():
            for b in range(NB):
                F[b * EXT + PAD - EDGE : b * EXT + PAD, :] = rtop[n, b]

    def corner_land(X, n, batches):
        above, below = batches

        def no_below():
            X[PAD + TR : PAD + TR + EDGE, :] = zero_pad

        def no_above():
            X[PAD - EDGE : PAD, :] = zero_pad

        above.land(no_below)
        below.land(no_above)

        @pl.when(bot_ok)
        def _():
            beyond = outer(pltpu.roll(rcorner[n, 3], HALF, 1), rcorner[n, 2])
            X[PAD + TR : PAD + TR + EDGE, :] = edges_of(rbot[n, 0], rbot[n, NB - 1], beyond)

        @pl.when(top_ok)
        def _():
            beyond = outer(pltpu.roll(rcorner[n, 1], HALF, 1), rcorner[n, 0])
            X[PAD - EDGE : PAD, :] = edges_of(rtop[n, 0], rtop[n, NB - 1], beyond)

    dinv_copies = halo_send(dv, 0)

    messages.land()

    def joined(pick):
        return jnp.concatenate([pick(t) for t in range(C)], axis=1)

    def places(pick):
        code = joined(pick).astype(jnp.int32)
        return divide(code, BC * C), remainder(code, BC)

    place_r = iota((BR, S), 0)
    place_c = iota((BC, S), 0)

    def one_hot(hit):
        return jnp.where(hit, 1.0, 0.0).astype(BF16)

    in_row, in_col = places(lambda t: msg_row[t, 1, 0:1, :])
    in_weight = joined(lambda t: msg_row[t, 1, 1:2, :])
    row_hit = place_r == in_row
    col_hot = one_hot(place_c == in_col)
    hot_own[...] = col_hot
    hi, lo = halves(cinit[0])
    seen = dot(hi, col_hot) + dot(lo, col_hot)
    at_via = jnp.sum(jnp.where(row_hit, seen, 0.0), axis=0, keepdims=True)
    for t in range(C):
        val_out[t] = at_via[:, t * per : (t + 1) * per]
    val_in[col] = val_out[col]
    values = Batch(always, always, val_in.at[pl.ds(0, C - 1)], [
        (val_out.at[lax.rem(col + d, C)], val_in.at[col], (row, lax.rem(col + d, C)))
        for d in range(1, C)
    ])

    messages_up = Batch(top_ok, bot_ok, msg_ud.at[1], [
        (msg_out.at[lax.rem(col + d, C) + 1], msg_ud.at[1, col], (up, lax.rem(col + d, C)))
        for d in range(C)
    ])
    messages_down = Batch(bot_ok, top_ok, msg_ud.at[0], [
        (msg_out.at[lax.rem(col + d, C) + 1], msg_ud.at[0, col], (down, lax.rem(col + d, C)))
        for d in range(C)
    ])

    dinv_corners = corner_send(0)

    cleak_load.wait()
    only = jnp.where(row_hit, in_weight, 0.0).astype(BF16)
    coarse_diag = 4.0 * coarse_conductance + cleak[...] + dot_t(only, col_hot)
    scale = relaxation / coarse_diag
    coarse_land(coarse0, 0, 1)
    volt = cinit[0]
    sides = beside(turn.at[0], R, C, volt, crow_top[0, 7:8, :], crow_bot[0, 0:1, :], cleft[0], cright[0])
    coarse[0] = volt + scale * (coarse_conductance * sides - coarse_diag * volt)
    coarse[1] = scale
    coarse[2] = coarse_diag
    for n in range(2):
        seams(coarse[n], n + 1)
    coarse_later = coarse_send(coarse.at[pl.ds(0, 2)], 1, 2)

    def quiet(ref, shape):
        def body():
            for t in range(C):
                ref[t] = jnp.zeros(shape, F32)
        return body

    left_row, left_col = places(lambda t: msg_row[t, 0, 0:1, :])
    right_row, right_col = places(lambda t: msg_row[t, 2, 0:1, :])
    hot_left[...] = one_hot(place_r == left_row)
    hot_right[...] = one_hot(place_r == right_row)

    def edge_copy(F, X, size):
        X[...] = edges_of(F[0:TR, :], F[(NB - 1) * size : (NB - 1) * size + TR, :], None)

    edge_copy(D, Dq, TR)
    halo_land(dv, dvq, 0, dinv_copies)

    for copy in amp_loads:
        copy.wait()
    values.land()
    drops = weight * joined(lambda o: val_in[o])
    drop_hi, drop_lo = halves(drops)
    half_step = TR

    def inject(i, carry):
        at = pl.ds(pl.multiple_of(i * half_step, half_step), half_step)
        hot = row_hot[at, :]
        added = dot(hot * drop_hi, Bt[...]) + dot(hot * drop_lo, Bt[...])
        for b in range(NB):
            inner = pl.ds(pl.multiple_of(b * EXT + PAD + i * half_step, 8), half_step)
            own = pl.ds(pl.multiple_of(b * TR + i * half_step, 8), half_step)
            value = amp[b, at, :] * mask[b, at, :].astype(F32) + added[:, b * LANES : (b + 1) * LANES]
            rhs[own, :] = value
            value = value * dv[inner, :]
            V[0, inner, :] = value
            woven[pl.ds((b * TR + i * half_step) * ITERS, half_step, stride=ITERS), :] = value
        return carry

    lax.fori_loop(0, TR // half_step, inject, 0)
    first_copies = halo_send(V.at[0], 1)
    corner_land(dvq, 0, dinv_corners)
    first_corners = corner_send(1)
    edge_copy(rhs, rhsq, TR)

    def stencil(k, start, size):
        place = wide(size)
        mids = [V[k, pl.ds(b * EXT + start, size), :] for b in range(NB)]
        lefts = [pltpu.roll(m, 1, 1) for m in mids]
        rights = [pltpu.roll(m, LANES - 1, 1) for m in mids]
        out = []
        for b in range(NB):
            tall = V[k, pl.ds(b * EXT + start - 1, size), :] + V[k, pl.ds(b * EXT + start + 1, size), :]
            before = jnp.where(place == 0, lefts[b - 1], lefts[b])
            after = jnp.where(place == LANES - 1, rights[(b + 1) % NB], rights[b])
            out.append(tall + (before + after))
        return mids, out

    def inward(b, value):
        place = wide(value.shape[0])
        if b == 0:
            value = jnp.where(place >= EDGE, value, 0.0)
        if b == NB - 1:
            value = jnp.where(place < LANES - EDGE, value, 0.0)
        return value

    def advance(k, start, size, totals, start0=None):
        start0 = start if start0 is None else start0
        mids, near = stencil(k, start, size)
        totals = None if totals is None else list(totals)
        for b in range(NB):
            at = pl.ds(b * EXT + start, size)
            own = pl.ds(b * TR + start - PAD, size)
            if k < ITERS - 1:
                fresh = dv[at, :] * near[b]
                if k:
                    fresh = (fresh + fresh) - V[k - 1, at, :]
                V[k + 1, at, :] = fresh
                if PAD <= start0 < PAD + TR:
                    woven[pl.ds((b * TR + start - PAD) * ITERS + k + 1, size, stride=ITERS), :] = fresh
                if totals is None:
                    continue
                if k == 0:
                    right_side = rhs[own, :]
                    applied = inward(b, right_side - near[b])
                    R0[own, :] = applied
                    totals[0] = totals[0] + fold(right_side * mids[b])
                    totals[1] = totals[1] + fold(applied * mids[b])
                    totals[2] = totals[2] + fold(applied * fresh)
                else:
                    totals[0] = totals[0] + fold(R0[own, :] * fresh)
            elif totals is not None:
                applied = inward(b, D[own, :] * mids[b] - near[b])
                totals[ITERS - 2] = totals[ITERS - 2] + fold(applied * mids[b])
                for j in range(1, ITERS - 1):
                    totals[j - 1] = totals[j - 1] + fold(applied * V[j, at, :])
        return None if totals is None else tuple(totals)

    def blank(n):
        return tuple(jnp.zeros((8, LANES), F32) for _ in range(n))

    kept = [3] + [1] * (ITERS - 2) + [ITERS - 1]
    inside = TR - 2 * EDGE
    chunk = inside
    piece = 8
    sums = []
    for k in range(ITERS):
        if k < ITERS - 1:
            advance(k, PAD, EDGE, None)
            advance(k, PAD + TR - EDGE, EDGE, None)

        def body(i, carry, k=k):
            for at in range(0, chunk, piece):
                carry = advance(k, PAD + EDGE + i * chunk + at, min(piece, chunk - at), carry, PAD)
            return carry

        sums.append(lax.fori_loop(0, inside // chunk, body, blank(kept[k])))

    halo_land(V.at[0], Q.at[0], 1, first_copies)
    corner_land(Q.at[0], 1, first_corners)
    def rim(value):
        place = wide(value.shape[0])
        ours = (place < EDGE) | ((place >= HALF - EDGE) & (place < HALF))
        return jnp.where(ours, value, 0.0)

    def advance_edge(k, start, size, totals):
        mid = Q[k, pl.ds(start, size), :]
        near = Q[k, pl.ds(start - 1, size), :] + Q[k, pl.ds(start + 1, size), :]
        near = near + (pltpu.roll(mid, 1, 1) + pltpu.roll(mid, LANES - 1, 1))
        at = pl.ds(start, size)
        own = pl.ds(start - PAD, size)
        totals = None if totals is None else list(totals)
        if k < ITERS - 1:
            fresh = dvq[at, :] * near
            if k:
                fresh = (fresh + fresh) - Q[k - 1, at, :]
            Q[k + 1, at, :] = fresh
            if totals is not None:
                if k == 0:
                    applied = rim(rhsq[own, :] - near)
                    rhsq[own, :] = applied
                    totals[1] = totals[1] + fold(applied * mid)
                    totals[2] = totals[2] + fold(applied * fresh)
                else:
                    totals[0] = totals[0] + fold(rhsq[own, :] * fresh)
        elif totals is not None:
            applied = rim(Dq[own, :] * mid - near)
            totals[ITERS - 2] = totals[ITERS - 2] + fold(applied * mid)
            for j in range(1, ITERS - 1):
                totals[j - 1] = totals[j - 1] + fold(applied * Q[j, at, :])
        return None if totals is None else tuple(totals)

    for k in range(ITERS):
        if k < ITERS - 1:
            advance(k, PAD - EDGE, EDGE, None)
            advance(k, PAD + TR, EDGE, None)
            advance_edge(k, PAD - EDGE, EDGE, None)
            advance_edge(k, PAD + TR, EDGE, None)
        sums[k] = advance(k, PAD, EDGE, sums[k])
        sums[k] = advance(k, PAD + TR - EDGE, EDGE, sums[k])
        sums[k] = advance_edge(k, PAD, TR, sums[k])

    flat = [total for part in sums for total in part]
    tile = jnp.concatenate([jnp.sum(total, axis=0, keepdims=True) for total in flat], axis=0)
    sub = iota((8, LANES), 0)
    number = len(flat)
    tile = jnp.sum(tile, axis=1, keepdims=True)
    red_out[...] = jnp.sum(jnp.where(sub == lane_row, tile, 0.0), axis=0, keepdims=True)
    me = row * C + col
    early = len(pending)
    red_in[me] = red_out[...]
    reductions = Batch(always, always, red_in.at[pl.ds(0, R * C - 1)], [
        (red_out, red_in.at[me], (lax.rem(row + e, R), lax.rem(col + d, C)))
        for e in reversed(range(R)) for d in reversed(range(C)) if e or d
    ])

    size = 64 if TR % 64 == 0 else EDGE
    for k in range(1, ITERS):
        for at in range(0, TR, size):
            edge = Q[k, PAD + at : PAD + at + size, :]
            place = wide(size)
            for b, value in ((0, edge), (NB - 1, pltpu.roll(edge, HALF, 1))):
                ours = place < EDGE if b == 0 else place >= LANES - EDGE
                here = pl.ds(b * EXT + PAD + at, size)
                value = jnp.where(ours, value, V[k, here, :])
                V[k, here, :] = value
                woven[pl.ds((b * TR + at) * ITERS + k, size, stride=ITERS), :] = value
    spot_copy.wait()
    diag_hit = iota((per, LANES), 0) == iota((per, LANES), 1)

    def pick(o):
        for s in range(o * per, (o + 1) * per):
            picked[s * ITERS : (s + 1) * ITERS, :] = woven[pl.ds(spot[0, s], ITERS), :]

    def lanes_of(o):
        hot = lane_hot[o * per : (o + 1) * per, :]
        for k in range(ITERS):
            mine = picked[pl.ds(o * per * ITERS + k, per, stride=ITERS), :]
            value = jnp.sum(mine * hot, axis=1, keepdims=True)
            seen_out[o + 1, k : k + 1, :] = jnp.sum(jnp.where(diag_hit, value, 0.0), axis=0, keepdims=True)

    for o in range(C + 1):
        if o < C:
            pick(o)
        if o:
            lanes_of(o - 1)
    seen_out[0] = seen_out[C]
    seen_out[C + 1] = seen_out[1]
    seen_row[col] = seen_out[pl.ds(col, 3)]
    seen_side = Batch(always, always, seen_row.at[pl.ds(0, C - 1)], [
        (seen_out.at[pl.ds(lax.rem(col + d, C), 3)], seen_row.at[col], (row, lax.rem(col + d, C)))
        for d in range(1, C)
    ])
    seen_up = Batch(top_ok, bot_ok, seen_ud.at[1], [
        (seen_out.at[lax.rem(col + d, C) + 1], seen_ud.at[1, col], (up, lax.rem(col + d, C)))
        for d in range(C)
    ])
    seen_down = Batch(bot_ok, top_ok, seen_ud.at[0], [
        (seen_out.at[lax.rem(col + d, C) + 1], seen_ud.at[0, col], (down, lax.rem(col + d, C)))
        for d in range(C)
    ])

    messages_down.land(quiet(msg_ud.at[0], (2, per)))
    messages_up.land(quiet(msg_ud.at[1], (2, per)))
    above_row, above_col = places(lambda t: msg_ud[0, t, 0:1, :])
    below_row, below_col = places(lambda t: msg_ud[1, t, 0:1, :])
    hot_up[...] = one_hot(place_c == above_col)
    hot_down[...] = one_hot(place_c == below_col)


    coarse_land(coarse_later, 1, 2)
    beyond_rows[0] = crow_top[1:3]
    beyond_rows[1] = crow_bot[1:3]
    beyond_cols[0] = cleft[1:3]
    beyond_cols[1] = cright[1:3]
    own_row, own_col = places(lambda t: msg_row[t, 1, 0:1, :])
    for n, part in enumerate((own_row, left_col, right_col, above_row, below_row)):
        nodes[n : n + 1, :] = part
    seen_side.land()
    seen_down.land(quiet(seen_ud.at[0], (ITERS, per)))
    seen_up.land(quiet(seen_ud.at[1], (ITERS, per)))
    heard = (
        (lambda t: seen_row[t, 1], lambda t: msg_row[t, 1, 1:2, :]),
        (lambda t: seen_row[t, 0], lambda t: msg_row[t, 0, 1:2, :]),
        (lambda t: seen_row[t, 2], lambda t: msg_row[t, 2, 1:2, :]),
        (lambda t: seen_ud[0, t], lambda t: msg_ud[0, t, 1:2, :]),
        (lambda t: seen_ud[1, t], lambda t: msg_ud[1, t, 1:2, :]),
    )
    for n, (seen, weights) in enumerate(heard):
        for t in range(C):
            basis[n, :, t * per : (t + 1) * per] = seen(t) * weights(t)

    for batch in pending[:early]:
        batch.leave()
    reductions.land()
    parts = [red_in[n] for n in range(R * C)]
    while len(parts) > 1:
        parts = [sum(parts[n : n + 2][1:], parts[n]) for n in range(0, len(parts), 2)]
    total = jnp.broadcast_to(parts[0], (8, LANES))
    total = jnp.sum(jnp.where(sub == lane_row, total, 0.0), axis=1, keepdims=True)
    scalar = [total[n : n + 1, :] for n in range(number)]
    energy = [scalar[1], scalar[2]] + scalar[3 : 3 + ITERS - 2]
    high = scalar[3 + ITERS - 2 :]
    for j in range(1, ITERS):
        energy.append(2.0 * high[j - 1] - energy[ITERS - 1 - j])
    moment = [scalar[0], scalar[0] - energy[0]]
    for n in range(2, ITERS):
        moment.append(2.0 * (moment[n - 1] - energy[n - 1]) - moment[n - 2])
    matrix = [[None] * (ITERS + 1) for _ in range(ITERS)]
    for j in range(ITERS):
        for k in range(j + 1):
            matrix[j][k] = matrix[k][j] = 0.5 * (energy[j + k] + energy[j - k])
        matrix[j][ITERS] = moment[j]
    for i in range(ITERS):
        inverse = 1.0 / matrix[i][i]
        for k in range(i + 1, ITERS + 1):
            matrix[i][k] = matrix[i][k] * inverse
        for j in range(i + 1, ITERS):
            for k in range(i + 1, ITERS + 1):
                matrix[j][k] = matrix[j][k] - matrix[j][i] * matrix[i][k]
    coef = [None] * ITERS
    for i in reversed(range(ITERS)):
        coef[i] = matrix[i][ITERS]
        for k in range(i + 1, ITERS):
            coef[i] = coef[i] - matrix[i][k] * coef[k]
    for k in range(ITERS):
        coef[k] = jnp.broadcast_to(coef[k], (1, LANES))
        coef_out[k : k + 1, :] = coef[k]
    for at in range(0, TR, 8):
        for b in range(NB):
            inner = pl.ds(b * EXT + PAD + at, 8)
            value = coef[0] * V[0, inner, :]
            for k in range(1, ITERS):
                value = value + coef[k] * V[k, inner, :]
            x_out[at : at + 8, b * LANES : (b + 1) * LANES] = value
    assert count[0] == send_sem.shape[0]
    for batch in pending[early:]:
        batch.leave()


def finish(
    R, C, x, coef, nodes, basis, coarse, beyond_rows, beyond_cols,
    hot_own, hot_left, hot_right, hot_up, hot_down,
    x_out, c_out, c, turn, sem,
):
    store = pltpu.make_async_copy(x, x_out, sem.at[0])
    store.start()
    BR, BC = c.shape
    S = basis.shape[2]
    groups = BC // GROUP
    by = [jnp.concatenate([coef[k : k + 1, :]] * (S // LANES), axis=1) for k in range(ITERS)]

    def gathered(n, hit, hot):
        amount = by[0] * basis[n, 0:1, :]
        for k in range(1, ITERS):
            amount = amount + by[k] * basis[n, k : k + 1, :]
        out = dot_t(spread(hit, amount), hot[...])
        return out[: out.shape[0] // 2] + out[out.shape[0] // 2 :]

    place_g = iota((groups, S), 0) * GROUP
    one_row = iota((8, S), 0) == 0
    on_left = gathered(1, place_g + (GROUP - 1) == nodes[1:2, :], hot_left)
    on_right = gathered(2, place_g == nodes[2:3, :], hot_right)
    on_above = gathered(3, one_row & (nodes[3:4, :] == BR - 1), hot_up)
    on_below = gathered(4, one_row & (nodes[4:5, :] == 0), hot_down)
    sources = gathered(0, iota((BR, S), 0) == nodes[0:1, :], hot_own)
    scale = coarse[1]
    volt = coarse[0] + scale * sources
    sides = beside(
        turn, R, C, volt,
        beyond_rows[0, 0, 7:8, :] + beyond_rows[0, 1, 7:8, :] * on_above[0:1, :],
        beyond_rows[1, 0, 0:1, :] + beyond_rows[1, 1, 0:1, :] * on_below[0:1, :],
        beyond_cols[0, 0] + beyond_cols[0, 1] * on_left,
        beyond_cols[1, 0] + beyond_cols[1, 1] * on_right,
    )
    c[...] = volt + scale * (sources + coarse_conductance * sides - coarse[2] * volt)
    last = pltpu.make_async_copy(c, c_out, sem.at[1])
    last.start()
    store.wait()
    last.wait()


def per_device(R, C, load_amp, load_mask, leak, coarse_leak, coarse_init, via_fine, via_coarse, via_count):
    inputs = (load_amp, load_mask, leak, coarse_leak, coarse_init, via_fine, via_coarse, via_count)
    TR, TC = leak.shape
    BR, BC = coarse_leak.shape
    S = via_fine.shape[1]
    per = S // C
    NB = TC // LANES
    EXT = TR + 2 * PAD
    groups = BC // GROUP
    batches = 24
    vmem = pl.BlockSpec(memory_space=pltpu.VMEM)
    state = pl.pallas_call(
        functools.partial(kernel, R, C),
        out_shape=(
            pltpu.VMEM((TR, TC), F32), pltpu.VMEM((8, LANES), F32), pltpu.VMEM((8, S), jnp.int32),
            pltpu.VMEM((5, ITERS, S), F32), pltpu.VMEM((3, BR, BC), F32),
            pltpu.VMEM((2, 2, 8, BC), F32), pltpu.VMEM((2, 2, groups, BR), F32),
            pltpu.VMEM((BC, S), BF16), pltpu.VMEM((BR, S), BF16), pltpu.VMEM((BR, S), BF16),
            pltpu.VMEM((BC, S), BF16), pltpu.VMEM((BC, S), BF16),
        ),
        in_specs=[pl.BlockSpec(memory_space=pltpu.HBM)] * 8,
        out_specs=(vmem,) * 12,
        scratch_shapes=[
            pltpu.VMEM((NB, TR, LANES), F32), pltpu.VMEM((NB, TR, LANES), jnp.int32),
            pltpu.VMEM((NB, TR, LANES), F32),
            pltpu.VMEM((BR, BC), F32), pltpu.VMEM((1, BR, BC), F32),
            pltpu.VMEM((1, S), jnp.int32), pltpu.VMEM((1, S), jnp.int32),
            pltpu.SMEM((1, C), jnp.int32), pltpu.SemaphoreType.DMA((9,)),
            pltpu.VMEM((C + 2, 2, per), F32), pltpu.VMEM((C, 3, 2, per), F32), pltpu.VMEM((2, C, 2, per), F32),
            pltpu.VMEM((C, 1, per), F32), pltpu.VMEM((C, 1, per), F32),
            pltpu.VMEM((C + 2, ITERS, per), F32), pltpu.VMEM((C, 3, ITERS, per), F32),
            pltpu.VMEM((2, C, ITERS, per), F32),
            pltpu.VMEM((1, S), jnp.int32), pltpu.SMEM((1, S), jnp.int32),
            pltpu.VMEM((NB * TR * ITERS, LANES), F32),
            pltpu.VMEM((ITERS * S, LANES), F32), pltpu.VMEM((S, LANES), F32),
            pltpu.VMEM((TR, S), BF16),
            pltpu.VMEM((S, TC), BF16),
            pltpu.VMEM((NB * EXT, LANES), F32),
            pltpu.VMEM((NB * TR, LANES), F32),
            pltpu.VMEM((EXT, LANES), F32),
            pltpu.VMEM((TR, LANES), F32),
            pltpu.VMEM((ITERS, NB * EXT, LANES), F32),
            pltpu.VMEM((ITERS, EXT, LANES), F32),
            pltpu.VMEM((NB * TR, LANES), F32),
            pltpu.VMEM((NB * TR, LANES), F32),
            pltpu.VMEM((TR, LANES), F32),
            pltpu.VMEM((2, TR, LANES), F32),
            pltpu.VMEM((2, LANES, TR), F32),
            pltpu.VMEM((2, LANES, TR), F32),
            pltpu.VMEM((2, NB, EDGE, LANES), F32),
            pltpu.VMEM((2, NB, EDGE, LANES), F32),
            pltpu.VMEM((2, 4, EDGE, LANES), F32),
            pltpu.VMEM((1, LANES), F32), pltpu.VMEM((R * C, 1, LANES), F32),
            pltpu.VMEM((3, BC, BR), F32), pltpu.VMEM((3, 2, groups, BR), F32),
            pltpu.VMEM((3, 8, BC), F32), pltpu.VMEM((3, 8, BC), F32),
            pltpu.VMEM((3, groups, BR), F32), pltpu.VMEM((3, groups, BR), F32),
            pltpu.SemaphoreType.DMA((batches,)),
            pltpu.SemaphoreType.DMA((batches,)),
        ],
        compiler_params=pltpu.CompilerParams(
            collective_id=0, has_side_effects=True, vmem_limit_bytes=40000 * 1024
        ),
    )(*(pltpu.with_memory_space_constraint(v, pltpu.HBM) for v in inputs))
    return pl.pallas_call(
        functools.partial(finish, R, C),
        out_shape=(jax.ShapeDtypeStruct((TR, TC), F32), jax.ShapeDtypeStruct((BR, BC), F32)),
        in_specs=[vmem] * 12,
        out_specs=(pl.BlockSpec(memory_space=pltpu.HBM),) * 2,
        scratch_shapes=[
            pltpu.VMEM((BR, BC), F32), pltpu.VMEM((BC, BR), F32), pltpu.SemaphoreType.DMA((2,)),
        ],
        compiler_params=pltpu.CompilerParams(vmem_limit_bytes=16000 * 1024),
    )(*(pltpu.with_memory_space_constraint(v, pltpu.VMEM) for v in state))


def solution(mesh):
    spec = P("row", "col")
    return jax.shard_map(
        functools.partial(per_device, mesh.shape["row"], mesh.shape["col"]),
        mesh=mesh, in_specs=(spec,) * 8, out_specs=(spec, spec), check_vma=False,
    )
```
